32 devices in a mesh: row: 8 (over z, core), col: 4 (over y, x).
Axes of the slice: x: 2, y: 2, z: 4, core: 2. Of those that a mesh axis runs over, the one named last changes fastest.
Arguments:
- flow_tiles: bfloat16 [8, 8, 256, 256], P('row', 'col'), may hold values from 0.1 to 25
- tile_cols: int32 [8, 8], P('row', 'col'), may hold values from -1 to 7, as said below
- pairs: int32 [512, 2], P(('row', 'col')), may hold values from -1 to 7, as said below
Outputs:
- new_flow: float32 [8, 8, 256, 256], P('row', 'col')
The draws below stay inside these ranges and needn't reach their ends.
Inputs may be any that keep to these rules, and one draw needn't show every extreme that they name: `tile_cols`: the stored slots of device (r, c) have distinct tile columns, each congruent to c modulo the col axis's size; tile row r stores tile column r. `pairs`: device (r, c) lists, in some order and without repeats, exactly the (k, s) for which slot s of the device is stored and M[r, k] and M[k, tile_cols[r, c * 2 + s]] are both stored tiles; its other rows are (-1, -1). Some device uses all 16 rows.
All inputs are finite; a program needn't handle non-finite values.
Results may differ from the reference program's by a relative error of at most 0.0003.
Values may be sent and summed in bfloat16 or wider, within the bound.
A program may use at most 64 MiB of HBM per device.

```python
import jax
import jax.numpy as jnp
from jax import lax

B = 256
NB = 8
TPD = 2
PPD = 16
N_COL = 4


def draw_flow_tiles(key, part):
    second_key = jax.random.fold_in(key, 1)
    row_values = jnp.arange(NB, dtype=jnp.float32)
    row_scale = 3.0 ** (row_values / jnp.float32(max(NB - 1, 1)))
    normal_part = jnp.clip(jax.random.normal(second_key, (NB, NB, B, B), jnp.float32), -4.0, 4.0)
    magnitude = jnp.exp(0.5 * normal_part)
    return (magnitude * row_scale[:, None, None, None]).astype(jnp.bfloat16)


def block_pattern(key):
    perm_key, keep_key, row_key, col_key = jax.random.split(jax.random.fold_in(key, 11), 4)
    subkeys = jax.random.split(perm_key, NB * N_COL)
    orders = jax.vmap(lambda subkey: jax.random.permutation(subkey, TPD))(subkeys)
    columns = jnp.arange(N_COL, dtype=jnp.int32)[None, :, None] + N_COL * orders.reshape(NB, N_COL, TPD).astype(jnp.int32)
    columns = columns.reshape(NB, NB).astype(jnp.int32)
    keep = jax.random.randint(keep_key, (NB, NB), 0, 2).astype(jnp.int32) > 0
    special_row = jax.random.randint(row_key, (), 0, NB).astype(jnp.int32)
    special_col = jax.random.randint(col_key, (), 0, N_COL).astype(jnp.int32)
    special_cols = jax.lax.dynamic_slice_in_dim(columns[special_row], special_col * TPD, TPD, 0)
    indices = jnp.arange(NB, dtype=jnp.int32)
    is_special_col = jnp.any(special_cols[None, :] == indices[:, None], axis=1)
    stored = keep | (indices[:, None] == indices[None, :]) | (indices[:, None] == special_row) | is_special_col[None, :]
    slot_stored = jnp.take_along_axis(stored, columns, axis=1)
    tile_cols = jnp.where(slot_stored, columns, -1).astype(jnp.int32)
    return (columns, stored, tile_cols)


def draw_tile_cols(key, part):
    columns, stored, tile_cols = block_pattern(key)
    return tile_cols


def draw_pairs(key, part):
    columns, stored, tile_cols = block_pattern(key)
    device_cols = columns.reshape(NB, N_COL, TPD)
    slot_stored = tile_cols.reshape(NB, N_COL, TPD) >= 0
    left_ok = stored[:, None, None, :]
    right_ok = stored.T[device_cols]
    valid = slot_stored[:, :, :, None] & left_ok & right_ok
    valid = valid.reshape(NB, N_COL, PPD)
    index_list = jnp.arange(PPD, dtype=jnp.int32)
    score = jnp.where(valid, index_list, index_list + PPD).astype(jnp.int32)
    order = jnp.argsort(score, axis=-1).astype(jnp.int32)
    valid_sorted = jnp.take_along_axis(valid, order, axis=-1)
    inner_tile = jnp.where(valid_sorted, order % NB, -1)
    slot_table = jnp.where(valid_sorted, order // NB, -1)
    return jnp.stack([inner_tile, slot_table], axis=-1).reshape(NB * N_COL * PPD, 2).astype(jnp.int32)


def setup_inputs(seed: int = 0) -> dict:
    keys = jax.random.split(jax.random.key(seed), 4)
    return {
        "flow_tiles": draw_flow_tiles(jax.random.fold_in(keys[3], 71), 0),
        "tile_cols": draw_tile_cols(jax.random.fold_in(keys[3], 71), 0),
        "pairs": draw_pairs(jax.random.fold_in(keys[3], 71), 0),
    }


def reference(flow_tiles, tile_cols, pairs):
    column_ids = jnp.arange(NB, dtype=jnp.int32)
    matching = tile_cols[:, None, :] == column_ids[None, :, None]
    present = jnp.any(matching, axis=2)
    position = jnp.argmax(matching, axis=2).astype(jnp.int32)
    taken = jnp.take_along_axis(flow_tiles, position[:, :, None, None], axis=1)
    ordered = jnp.where(present[:, :, None, None], taken, jnp.zeros((), flow_tiles.dtype))
    pair_table = pairs.reshape(NB, N_COL, PPD, 2)
    slot_ids = jnp.arange(TPD, dtype=jnp.int32)

    def one_row(row_id):
        def one_device(col_id):
            inner_tile = pair_table[row_id, col_id, :, 0]
            slot_list = pair_table[row_id, col_id, :, 1]
            is_live = inner_tile >= 0
            inner_safe = jnp.maximum(inner_tile, 0)
            slot_safe = jnp.maximum(slot_list, 0)
            wanted = jnp.maximum(tile_cols[row_id, col_id * TPD + slot_safe], 0)
            left_tiles = ordered[row_id, inner_safe].astype(jnp.float32)
            right_tiles = ordered[inner_safe, wanted].astype(jnp.float32)
            products = jnp.einsum('pab,pbc->pac', left_tiles, right_tiles, precision=lax.Precision.HIGHEST)
            weight = (is_live[:, None] & (slot_list[:, None] == slot_ids[None, :])).astype(jnp.float32)
            return jnp.einsum('ps,pac->sac', weight, products, precision=lax.Precision.HIGHEST)
        return lax.map(one_device, jnp.arange(N_COL, dtype=jnp.int32))

    expanded = lax.map(one_row, jnp.arange(NB, dtype=jnp.int32)).reshape(NB, NB, B, B)
    inflated = expanded * expanded
    inflated_ordered = jnp.take_along_axis(inflated, position[:, :, None, None], axis=1)
    inflated_ordered = jnp.where(present[:, :, None, None], inflated_ordered, 0.0)
    totals = jnp.sum(inflated_ordered, axis=(0, 2))
    stored = tile_cols >= 0
    divisor = totals[jnp.maximum(tile_cols, 0)]
    divisor = jnp.where(stored[:, :, None], divisor, 1.0)
    normed = inflated * jnp.float32(NB * B) / divisor[:, :, None, :]
    blended = 0.5 * flow_tiles.astype(jnp.float32) + 0.5 * normed
    return jnp.where(stored[:, :, None, None], blended, 0.0)
```

```python
import functools
import math

import jax
import jax.numpy as jnp
from jax import lax
from jax.experimental import pallas as pl
from jax.experimental.pallas import tpu as pltpu
from jax.sharding import PartitionSpec as P

MESH = pl.DeviceIdType.MESH
CORES = 2
SPLIT = 2


def remote(src, dst, send_sem, recv_sem, device):
    return pltpu.make_async_remote_copy(
        src_ref=src,
        dst_ref=dst,
        send_sem=send_sem,
        recv_sem=recv_sem,
        device_id=device,
        device_id_type=MESH,
    )


def kernel(
    nrow, ncol, cols_hbm, flow_hbm, out_ref,
    cols, raw, own, blocks, left, acc, swap, result, flags, sums,
    in_sem, up_send, dn_send, mate_send, recv, left_send, left_recv,
    left_mate, flag_sem, swap_sem, sum_send, sum_recv,
):
    tiles, width = raw.shape[0], raw.shape[2]
    depth = own.shape[1]
    share = tiles // CORES
    pieces = share * SPLIT
    planes = nrow // CORES
    row, col = lax.axis_index("row"), lax.axis_index("col")
    z, core = row // CORES, row % CORES
    mate = (row + 1 - 2 * core, col)
    mate_row = row + 1 - 2 * core
    above, below = (row + CORES, col), (row - CORES, col)
    has_above, has_below = z < planes - 1, z > 0
    ny = math.isqrt(ncol)
    ny = ny if ny * ny == ncol else 1
    nx = ncol // ny
    y, x = col // nx, col % nx
    half = tiles // 2

    def at(dy, dx):
        return ((y + dy) % ny) * nx + (x + dx) % nx

    along_x = [(0, dx) for dx in range(1, nx)]
    along_y = [(dy, 0) for dy in range(1, ny)]
    across = [(dy, dx) for dy, _ in along_y for _, dx in along_x]

    load_cols = pltpu.make_async_copy(cols_hbm, cols, in_sem.at[0])
    load_flow = pltpu.make_async_copy(flow_hbm.at[0], raw, in_sem.at[1])
    load_cols.start()
    load_flow.start()

    barrier = pltpu.get_barrier_semaphore()

    def greet(device):
        pl.semaphore_signal(barrier, inc=1, device_id=device, device_id_type=MESH)

    greet(mate)
    for d in along_x + along_y:
        greet((row, at(*d)))

    @pl.when(has_above)
    def _():
        for c in range(CORES):
            greet(((z + 1) * CORES + c, col))

    @pl.when(has_below)
    def _():
        for c in range(CORES):
            greet(((z - 1) * CORES + c, col))

    load_cols.wait()
    load_flow.wait()
    for t in range(tiles):
        target = col + ncol * t
        tile = jnp.zeros((width, width), jnp.float32)
        weight = jnp.float32(0)
        for s in range(tiles):
            w = (cols[0, s] == target).astype(jnp.float32)
            weight = weight + w
            tile = tile + raw[s].astype(jnp.float32) * w
        flags[core, t] = jnp.full((width,), weight, jnp.float32)
        tile = tile.astype(jnp.bfloat16)
        own[t * SPLIT:(t + 1) * SPLIT] = tile.reshape(SPLIT, depth, width)
        left[col, t, core] = tile
    blocks[row] = own[pl.ds(core * pieces, pieces)]

    ends = jnp.where(has_above, 1, 0) + jnp.where(has_below, 1, 0)
    pl.semaphore_wait(barrier, nx + ny - 1 + CORES * ends)

    def piece(src, k, u, send_sem, device):
        return remote(src, blocks.at[k, u], send_sem, recv.at[k, u], device)

    def arrived(k, u):
        piece(own.at[u], k, u, mate_send.at[u], mate).wait_recv()

    def to_mate(u):
        return piece(own.at[(1 - core) * pieces + u], row, u, mate_send.at[u], mate)

    def left_copy(c, t, rc, device, send_sem):
        part = left.at[c, t, rc]
        return remote(part, part, send_sem, left_recv.at[rc, c, t], device)

    def left_out(source, move, t):
        slot = (source[0] + move[0]) * nx + source[1] + move[1]
        return left_copy(at(*source), t, core, (row, at(*move)), left_send.at[slot, t])

    def left_to_mate(source, t):
        c = at(*source)
        return left_copy(c, t, core, mate, left_mate.at[c, t])

    def left_arrived(source, t):
        left_to_mate(source, t).wait_recv()
        left_to_mate(source, t).start()

    def left_relay():
        for t in range(half):
            for d in along_x:
                left_arrived(d, t)
                for move in along_y:
                    left_out(d, move, t).start()
        for t in range(half, tiles):
            for d in along_y:
                left_arrived(d, t)
                for move in along_x:
                    left_out(d, move, t).start()

    flag_copy = remote(flags.at[core], flags.at[core], flag_sem.at[0], flag_sem.at[1], mate)

    for u in range(pieces):
        for c in range(CORES):

            @pl.when(has_above)
            def _():
                piece(
                    own.at[c * pieces + u], row, u, up_send.at[0, c * pieces + u],
                    ((z + 1) * CORES + c, col),
                ).start()

            @pl.when(has_below)
            def _():
                piece(
                    own.at[c * pieces + u], row, u, dn_send.at[0, c * pieces + u],
                    ((z - 1) * CORES + c, col),
                ).start()

        if u == 0:
            for t in range(tiles):
                for d in along_x:
                    left_out((0, 0), d, t).start()
                for d in along_y:
                    left_out((0, 0), d, tiles - 1 - t).start()
    for u in range(pieces):
        to_mate(u).start()
    for t in range(tiles):
        left_to_mate((0, 0), t).start()
    flag_copy.start()

    acc[...] = jnp.zeros_like(acc)

    def relay(step):
        for c in range(CORES):
            if step == 1 and c == CORES - 1:
                left_relay()
            for u in range(pieces):

                @pl.when(z >= step)
                def _():
                    k = (z - step) * CORES + c
                    arrived(k, u)

                    @pl.when(has_above)
                    def _():
                        piece(
                            blocks.at[k, u], k, u, up_send.at[step, c * pieces + u], above
                        ).start()

                @pl.when(z + step < planes)
                def _():
                    k = (z + step) * CORES + c
                    arrived(k, u)

                    @pl.when(has_below)
                    def _():
                        piece(
                            blocks.at[k, u], k, u, dn_send.at[step, c * pieces + u], below
                        ).start()

    def multiply(k):
        a = left[k % ncol, k // ncol].reshape(CORES * width, width)
        for i in range(share):
            b = blocks[k, pl.ds(i * SPLIT, SPLIT)].reshape(width, width)
            c = jnp.dot(a, b, preferred_element_type=jnp.float32)
            acc[i] += c.reshape(CORES, width, width)

    def multiply_piece(k, u):
        h = u % SPLIT
        a = left[k % ncol, k // ncol, :, :, pl.ds(h * depth, depth)]
        c = jnp.dot(
            a.reshape(CORES * width, depth), blocks[k, u], preferred_element_type=jnp.float32
        )
        acc[u // SPLIT] += c.reshape(CORES, width, width)

    def compute(distance):
        for sign in (-1, 1) if distance else (1,):
            plane = z + sign * distance

            @pl.when((plane >= 0) & (plane < planes))
            def _():
                if distance == 0:
                    for u in range(pieces):
                        arrived(mate_row, u)
                for c in range(CORES):
                    multiply(plane * CORES + c)

    def last(distance):
        for sign in (-1, 1):
            plane = z + sign * distance

            @pl.when((plane >= 0) & (plane < planes))
            def _():
                for c in range(CORES):
                    for u in range(pieces):
                        k = plane * CORES + c
                        arrived(k, u)
                        multiply_piece(k, u)

    done = 0

    def catch_up(upto):
        nonlocal done
        if done == 0:
            for d in across:
                for t in range(tiles):
                    left_arrived(d, t)
            for c in range(ncol):
                for t in range(tiles):
                    left_copy(c, t, 1 - core, mate, left_mate.at[c, t]).wait_recv()
        while done < upto:
            compute(done)
            done += 1

    for step in range(1, planes - 1):
        if step > 2:
            catch_up(step)
        relay(step)
        if step == 1:
            for t in range(half, tiles):
                for d in along_x:
                    left_arrived(d, t)
            for t in range(half):
                for d in along_y:
                    left_arrived(d, t)
    catch_up(planes - 1)
    last(planes - 1)
    flag_copy.wait_recv()

    for i in range(share):
        t = core * share + i
        part = jnp.zeros((width,), jnp.float32)
        for c in range(CORES):
            part = part + jnp.sum(acc[i, c] * acc[i, c], axis=0) * flags[c, t]
        sums[row, i] = part

    def to_row(d):
        return remote(
            sums.at[row], sums.at[row], sum_send.at[d], sum_recv.at[row],
            ((row + d) % nrow, col),
        )

    for d in range(1, nrow):
        to_row(d).start()

    for i in range(share):
        other = acc[i, 1 - core]
        swap[i] = other * other
    swap_copy = remote(
        swap, result.at[pl.ds(core * share, share)], swap_sem.at[0], swap_sem.at[1], mate
    )
    swap_copy.start()
    for i in range(share):
        mine = acc[i, core]
        result[core * share + i] = mine * mine
    swap_copy.wait_recv()

    for d in range(1, nrow):
        other = (row + d) % nrow
        remote(
            sums.at[other], sums.at[other], sum_send.at[d], sum_recv.at[other], (other, col)
        ).wait_recv()
    for s in range(tiles):
        out = jnp.zeros((width, width), jnp.float32)
        held = jnp.float32(0)
        for t in range(tiles):
            w = (cols[0, s] == col + ncol * t).astype(jnp.float32)
            held = held + w
            total = sums[t // share, t % share]
            for p in range(1, planes):
                total = total + sums[p * CORES + t // share, t % share]
            safe = jnp.where(total > 0, total, 1.0)
            scale = jnp.float32(0.5 * nrow * width) / safe * w
            out = out + result[t] * scale[None, :]
        out_ref[0, s] = out + raw[s].astype(jnp.float32) * (0.5 * held)
    for n in range(CORES * pieces):
        for step in range(planes):

            @pl.when(has_above & (z >= step))
            def _():
                piece(own.at[n], row, 0, up_send.at[step, n], above).wait_send()

            @pl.when(has_below & (z + step < planes))
            def _():
                piece(own.at[n], row, 0, dn_send.at[step, n], below).wait_send()

    for u in range(pieces):
        to_mate(u).wait_send()
    for t in range(tiles):
        for d in along_x + along_y:
            left_out((0, 0), d, t).wait_send()
        for dy, dx in across:
            source, move = ((0, dx), (dy, 0)) if t < half else ((dy, 0), (0, dx))
            left_out(source, move, t).wait_send()
        for c in range(ncol):
            left_copy(c, t, core, mate, left_mate.at[c, t]).wait_send()
    flag_copy.wait_send()
    swap_copy.wait_send()
    for d in range(1, nrow):
        to_row(d).wait_send()


def on_device(nrow, ncol, flow_tiles, tile_cols, pairs):
    _, tiles, _, width = flow_tiles.shape
    planes, depth, share = nrow // CORES, width // SPLIT, tiles // CORES
    pieces = share * SPLIT
    dma = pltpu.SemaphoreType.DMA
    return pl.pallas_call(
        functools.partial(kernel, nrow, ncol),
        out_shape=jax.ShapeDtypeStruct(flow_tiles.shape, jnp.float32),
        in_specs=[pl.BlockSpec(memory_space=pltpu.HBM)] * 2,
        out_specs=pl.BlockSpec(memory_space=pltpu.VMEM),
        scratch_shapes=[
            pltpu.SMEM((1, tiles), jnp.int32),
            pltpu.VMEM((tiles, width, width), jnp.bfloat16),
            pltpu.VMEM((CORES * pieces, depth, width), jnp.bfloat16),
            pltpu.VMEM((nrow, pieces, depth, width), jnp.bfloat16),
            pltpu.VMEM((ncol, tiles, CORES, width, width), jnp.bfloat16),
            pltpu.VMEM((share, CORES, width, width), jnp.float32),
            pltpu.VMEM((share, width, width), jnp.float32),
            pltpu.VMEM((tiles, width, width), jnp.float32),
            pltpu.VMEM((CORES, tiles, width), jnp.float32),
            pltpu.VMEM((nrow, share, width), jnp.float32),
            dma((2,)),
            dma((planes, CORES * pieces)),
            dma((planes, CORES * pieces)),
            dma((pieces,)),
            dma((nrow, pieces)),
            dma((ncol, tiles)),
            dma((CORES, ncol, tiles)),
            dma((ncol, tiles)),
            dma((2,)),
            dma((2,)),
            dma((nrow,)),
            dma((nrow,)),
        ],
        compiler_params=pltpu.CompilerParams(
            collective_id=0, has_side_effects=True, vmem_limit_bytes=24 * 1024 * 1024
        ),
        name="cluster_step",
    )(
        pltpu.with_memory_space_constraint(tile_cols, pltpu.HBM),
        pltpu.with_memory_space_constraint(flow_tiles, pltpu.HBM),
    )


def solution(mesh):
    placed = (P("row", "col", None, None), P("row", "col"), P(("row", "col"), None))
    return jax.shard_map(
        functools.partial(on_device, mesh.shape["row"], mesh.shape["col"]),
        mesh=mesh,
        in_specs=placed,
        out_specs=P("row", "col", None, None),
        check_vma=False,
    )
```

```python
import functools
import math

import jax
import jax.numpy as jnp
from jax import lax
from jax.experimental import pallas as pl
from jax.experimental.pallas import tpu as pltpu
from jax.sharding import PartitionSpec as P

MESH = pl.DeviceIdType.MESH
CORES = 2
SPLIT = 2


def remote(src, dst, send_sem, recv_sem, device):
    return pltpu.make_async_remote_copy(
        src_ref=src,
        dst_ref=dst,
        send_sem=send_sem,
        recv_sem=recv_sem,
        device_id=device,
        device_id_type=MESH,
    )


def kernel(
    nrow, ncol, cols_hbm, flow_hbm, out_ref,
    cols, raw, own, blocks, left, acc, swap, result, flags, sums,
    in_sem, z_send, piece_sem, recv, left_send, left_recv, mate_sem,
    flag_sem, swap_sem, sum_sem,
):
    tiles, width = raw.shape[0], raw.shape[2]
    depth = own.shape[1]
    share = tiles // CORES
    pieces = share * SPLIT
    planes = nrow // CORES
    row, col = lax.axis_index("row"), lax.axis_index("col")
    z, core = row // CORES, row % CORES
    mate = (row + 1 - 2 * core, col)
    mate_row = row + 1 - 2 * core
    above, below = (row + CORES, col), (row - CORES, col)
    has_above, has_below = z < planes - 1, z > 0
    ny = math.isqrt(ncol)
    ny = ny if ny * ny == ncol else 1
    nx = ncol // ny
    y, x = col // nx, col % nx
    half = tiles // 2

    def at(dy, dx):
        return ((y + dy) % ny) * nx + (x + dx) % nx

    along_x = [(0, dx) for dx in range(1, nx)]
    along_y = [(dy, 0) for dy in range(1, ny)]
    across = [(dy, dx) for dy, _ in along_y for _, dx in along_x]

    load_cols = pltpu.make_async_copy(cols_hbm, cols, in_sem.at[0])
    load_flow = pltpu.make_async_copy(flow_hbm.at[0], raw, in_sem.at[1])
    load_cols.start()
    load_flow.start()

    barrier = pltpu.get_barrier_semaphore()

    def greet(device):
        pl.semaphore_signal(barrier, inc=1, device_id=device, device_id_type=MESH)

    greet(mate)
    for d in along_x + along_y:
        greet((row, at(*d)))

    @pl.when(has_above)
    def _():
        for c in range(CORES):
            greet(((z + 1) * CORES + c, col))

    @pl.when(has_below)
    def _():
        for c in range(CORES):
            greet(((z - 1) * CORES + c, col))

    load_cols.wait()
    load_flow.wait()
    for t in range(tiles):
        target = col + ncol * t
        tile = jnp.zeros((width, width), jnp.float32)
        weight = jnp.float32(0)
        for s in range(tiles):
            w = (cols[0, s] == target).astype(jnp.float32)
            weight = weight + w
            tile = tile + raw[s].astype(jnp.float32) * w
        flags[core, t] = jnp.full((width,), weight, jnp.float32)
        tile = tile.astype(jnp.bfloat16)
        own[t * SPLIT:(t + 1) * SPLIT] = tile.reshape(SPLIT, depth, width)
        left[col, t, core] = tile
    blocks[row] = own[pl.ds(core * pieces, pieces)]

    ends = jnp.where(has_above, 1, 0) + jnp.where(has_below, 1, 0)
    pl.semaphore_wait(barrier, nx + ny - 1 + CORES * ends)

    def piece(src, k, u, send_sem, device):
        return remote(src, blocks.at[k, u], send_sem, recv.at[k, u], device)

    def arrived(k, u):
        piece(own.at[u], k, u, piece_sem, mate).wait_recv()

    def to_mate(u):
        return piece(own.at[(1 - core) * pieces + u], row, u, piece_sem, mate)

    def left_out(source, move, t):
        c = at(*source)
        part = left.at[c, t, core]
        return remote(part, part, left_send, left_recv.at[c, t], (row, at(*move)))

    def left_to_mate(source, t):
        part = left.at[at(*source), t, core]
        return remote(part, part, mate_sem.at[0], mate_sem.at[1], mate)

    def left_from_mate():
        part = left.at[:, :, 1 - core]
        return remote(part, part, mate_sem.at[0], mate_sem.at[1], mate)

    def left_arrived(source, t):
        left_out(source, source, t).wait_recv()
        left_to_mate(source, t).start()

    def left_relay():
        for t in range(half):
            for d in along_x:
                left_arrived(d, t)
                for move in along_y:
                    left_out(d, move, t).start()
        for t in range(half, tiles):
            for d in along_y:
                left_arrived(d, t)
                for move in along_x:
                    left_out(d, move, t).start()

    flag_copy = remote(flags.at[core], flags.at[core], flag_sem.at[0], flag_sem.at[1], mate)

    for u in range(pieces):
        for c in range(CORES):

            @pl.when(has_above)
            def _():
                piece(
                    own.at[c * pieces + u], row, u, z_send.at[0],
                    ((z + 1) * CORES + c, col),
                ).start()

            @pl.when(has_below)
            def _():
                piece(
                    own.at[c * pieces + u], row, u, z_send.at[1],
                    ((z - 1) * CORES + c, col),
                ).start()

        if u == 0:
            for t in range(tiles):
                for d in along_x:
                    left_out((0, 0), d, t).start()
                for d in along_y:
                    left_out((0, 0), d, tiles - 1 - t).start()
    for u in range(pieces):
        to_mate(u).start()
    for t in range(tiles):
        left_to_mate((0, 0), t).start()
    flag_copy.start()

    acc[...] = jnp.zeros_like(acc)

    def relay(step):
        for c in range(CORES):
            if step == 1 and c == CORES - 1:
                left_relay()
            for u in range(pieces):

                @pl.when(z >= step)
                def _():
                    k = (z - step) * CORES + c
                    arrived(k, u)

                    @pl.when(has_above)
                    def _():
                        piece(blocks.at[k, u], k, u, z_send.at[0], above).start()

                @pl.when(z + step < planes)
                def _():
                    k = (z + step) * CORES + c
                    arrived(k, u)

                    @pl.when(has_below)
                    def _():
                        piece(blocks.at[k, u], k, u, z_send.at[1], below).start()

    def multiply(k):
        a = left[k % ncol, k // ncol].reshape(CORES * width, width)
        for i in range(share):
            b = blocks[k, pl.ds(i * SPLIT, SPLIT)].reshape(width, width)
            c = jnp.dot(a, b, preferred_element_type=jnp.float32)
            acc[i] += c.reshape(CORES, width, width)

    def multiply_piece(k, u):
        h = u % SPLIT
        a = left[k % ncol, k // ncol, :, :, pl.ds(h * depth, depth)]
        c = jnp.dot(
            a.reshape(CORES * width, depth), blocks[k, u], preferred_element_type=jnp.float32
        )
        acc[u // SPLIT] += c.reshape(CORES, width, width)

    def compute(distance):
        for sign in (-1, 1) if distance else (1,):
            plane = z + sign * distance

            @pl.when((plane >= 0) & (plane < planes))
            def _():
                if distance == 0:
                    for u in range(pieces):
                        arrived(mate_row, u)
                for c in range(CORES):
                    multiply(plane * CORES + c)

    def last(distance):
        for sign in (-1, 1):
            plane = z + sign * distance

            @pl.when((plane >= 0) & (plane < planes))
            def _():
                for c in range(CORES):
                    for u in range(pieces):
                        k = plane * CORES + c
                        arrived(k, u)
                        multiply_piece(k, u)

    done = 0

    def catch_up(upto):
        nonlocal done
        if done == 0:
            for d in across:
                for t in range(tiles):
                    left_arrived(d, t)
            left_from_mate().wait_recv()
        while done < upto:
            compute(done)
            done += 1

    for step in range(1, planes - 1):
        if step > 2:
            catch_up(step)
        relay(step)
        if step == 1:
            for t in range(half, tiles):
                for d in along_x:
                    left_arrived(d, t)
            for t in range(half):
                for d in along_y:
                    left_arrived(d, t)
    catch_up(planes - 1)
    last(planes - 1)
    flag_copy.wait_recv()

    for i in range(share):
        t = core * share + i
        part = jnp.zeros((width,), jnp.float32)
        for c in range(CORES):
            part = part + jnp.sum(acc[i, c] * acc[i, c], axis=0) * flags[c, t]
        sums[row, i] = part

    def to_row(d):
        return remote(
            sums.at[row], sums.at[row], sum_sem.at[0], sum_sem.at[1],
            ((row + d) % nrow, col),
        )

    def all_sums():
        part = sums.at[pl.ds(0, nrow - 1)]
        return remote(part, part, sum_sem.at[0], sum_sem.at[1], mate)

    for d in range(1, nrow):
        to_row(d).start()

    for i in range(share):
        other = acc[i, 1 - core]
        swap[i] = other * other
    swap_copy = remote(
        swap, result.at[pl.ds(core * share, share)], swap_sem.at[0], swap_sem.at[1], mate
    )
    swap_copy.start()
    for i in range(share):
        mine = acc[i, core]
        result[core * share + i] = mine * mine
    swap_copy.wait_recv()

    all_sums().wait_recv()
    for s in range(tiles):
        out = jnp.zeros((width, width), jnp.float32)
        held = jnp.float32(0)
        for t in range(tiles):
            w = (cols[0, s] == col + ncol * t).astype(jnp.float32)
            held = held + w
            total = sums[t // share, t % share]
            for p in range(1, planes):
                total = total + sums[p * CORES + t // share, t % share]
            safe = jnp.where(total > 0, total, 1.0)
            scale = jnp.float32(0.5 * nrow * width) / safe * w
            out = out + result[t] * scale[None, :]
        out_ref[0, s] = out + raw[s].astype(jnp.float32) * (0.5 * held)
    def sent(number, sem):
        part = blocks.at[pl.ds(0, number * CORES)]
        remote(part, part, sem, sem, mate).wait_send()

    for p in range(planes):

        @pl.when(z == p)
        def _():
            if p < planes - 1:
                sent(p + 1, z_send.at[0])
            if p > 0:
                sent(planes - p, z_send.at[1])

    part = own.at[pl.ds(0, pieces)]
    remote(part, part, piece_sem, piece_sem, mate).wait_send()
    part = left.at[pl.ds(0, ncol - 1), :, core]
    remote(part, part, left_send, left_send, mate).wait_send()
    left_from_mate().wait_send()
    flag_copy.wait_send()
    swap_copy.wait_send()
    all_sums().wait_send()


def on_device(nrow, ncol, flow_tiles, tile_cols, pairs):
    _, tiles, _, width = flow_tiles.shape
    planes, depth, share = nrow // CORES, width // SPLIT, tiles // CORES
    pieces = share * SPLIT
    dma = pltpu.SemaphoreType.DMA
    return pl.pallas_call(
        functools.partial(kernel, nrow, ncol),
        out_shape=jax.ShapeDtypeStruct(flow_tiles.shape, jnp.float32),
        in_specs=[pl.BlockSpec(memory_space=pltpu.HBM)] * 2,
        out_specs=pl.BlockSpec(memory_space=pltpu.VMEM),
        scratch_shapes=[
            pltpu.SMEM((1, tiles), jnp.int32),
            pltpu.VMEM((tiles, width, width), jnp.bfloat16),
            pltpu.VMEM((CORES * pieces, depth, width), jnp.bfloat16),
            pltpu.VMEM((nrow, pieces, depth, width), jnp.bfloat16),
            pltpu.VMEM((ncol, tiles, CORES, width, width), jnp.bfloat16),
            pltpu.VMEM((share, CORES, width, width), jnp.float32),
            pltpu.VMEM((share, width, width), jnp.float32),
            pltpu.VMEM((tiles, width, width), jnp.float32),
            pltpu.VMEM((CORES, tiles, width), jnp.float32),
            pltpu.VMEM((nrow, share, width), jnp.float32),
            dma((2,)),
            dma((2,)),
            dma,
            dma((nrow, pieces)),
            dma,
            dma((ncol, tiles)),
            dma((2,)),
            dma((2,)),
            dma((2,)),
            dma((2,)),
        ],
        compiler_params=pltpu.CompilerParams(
            collective_id=0, has_side_effects=True, vmem_limit_bytes=24 * 1024 * 1024
        ),
        name="cluster_step",
    )(
        pltpu.with_memory_space_constraint(tile_cols, pltpu.HBM),
        pltpu.with_memory_space_constraint(flow_tiles, pltpu.HBM),
    )


def solution(mesh):
    placed = (P("row", "col", None, None), P("row", "col"), P(("row", "col"), None))
    return jax.shard_map(
        functools.partial(on_device, mesh.shape["row"], mesh.shape["col"]),
        mesh=mesh,
        in_specs=placed,
        out_specs=P("row", "col", None, None),
        check_vma=False,
    )
```

```python
import functools
import math

import jax
import jax.numpy as jnp
from jax import lax
from jax.experimental import pallas as pl
from jax.experimental.pallas import tpu as pltpu
from jax.sharding import PartitionSpec as P

MESH = pl.DeviceIdType.MESH
CORES = 2
SPLIT = 2


def remote(src, dst, send_sem, recv_sem, device):
    return pltpu.make_async_remote_copy(
        src_ref=src,
        dst_ref=dst,
        send_sem=send_sem,
        recv_sem=recv_sem,
        device_id=device,
        device_id_type=MESH,
    )


def kernel(
    nrow, ncol, cols_hbm, flow_hbm, out_ref,
    cols, raw, left, blocks, aid, acc, aid_acc, flags, aid_flags, sums,
    in_sem, z_send, mate_send, recv, mate_recv, left_send, left_recv,
    aid_send, aid_recv, flag_sem, sum_sem,
):
    tiles, width = raw.shape[0], raw.shape[2]
    depth = left.shape[3]
    planes = nrow // CORES
    row, col = lax.axis_index("row"), lax.axis_index("col")
    z, core = row // CORES, row % CORES
    mate_row = row + 1 - 2 * core
    mate = (mate_row, col)
    above, below = (row + CORES, col), (row - CORES, col)
    has_above, has_below = z < planes - 1, z > 0
    ny = math.isqrt(ncol)
    ny = ny if ny * ny == ncol else 1
    nx = ncol // ny
    y, x = col // nx, col % nx
    half = tiles // 2
    top = planes - 1
    is_end = (z == 0) | (z == top)
    is_inside = jnp.logical_not(is_end)
    is_aide = (z == 1) | (z == top - 1)
    end_row = jnp.where(z <= 1, 0, top) * CORES + core
    inner_row = jnp.where(z == 0, 1, top - 1) * CORES + core

    def at(dy, dx):
        return ((y + dy) % ny) * nx + (x + dx) % nx

    along_x = [(0, dx) for dx in range(1, nx)]
    along_y = [(dy, 0) for dy in range(1, ny)]
    beside = along_x + along_y
    across = [(dy, dx) for dy, _ in along_y for _, dx in along_x]
    firsts = [(d, t) for t in range(half) for d in along_x]
    firsts += [(d, t) for t in range(half, tiles) for d in along_y]
    seconds = [(d, t) for t in range(half, tiles) for d in along_x]
    seconds += [(d, t) for t in range(half) for d in along_y]

    load_cols = pltpu.make_async_copy(cols_hbm, cols, in_sem.at[0])
    load_flow = pltpu.make_async_copy(flow_hbm.at[0], raw, in_sem.at[1])
    load_cols.start()
    load_flow.start()

    barrier = pltpu.get_barrier_semaphore()

    def greet(device):
        pl.semaphore_signal(barrier, inc=1, device_id=device, device_id_type=MESH)

    greet(mate)
    for d in beside:
        greet((row, at(*d)))
        greet((mate_row, at(*d)))

    @pl.when(has_above)
    def _():
        for c in range(CORES):
            greet(((z + 1) * CORES + c, col))

    @pl.when(has_below)
    def _():
        for c in range(CORES):
            greet(((z - 1) * CORES + c, col))

    load_cols.wait()
    load_flow.wait()
    for t in range(tiles):
        target = col + ncol * t
        tile = jnp.zeros((width, width), jnp.float32)
        weight = jnp.float32(0)
        for s in range(tiles):
            w = (cols[0, s] == target).astype(jnp.float32)
            weight = weight + w
            tile = tile + raw[s].astype(jnp.float32) * w
        flags[t] = jnp.full((width,), weight, jnp.float32)
        tile = tile.astype(jnp.bfloat16).reshape(SPLIT, depth, width)
        left[col, t] = tile
        blocks[row, t] = tile

    ends = jnp.where(has_above, 1, 0) + jnp.where(has_below, 1, 0)
    pl.semaphore_wait(barrier, 1 + CORES * (len(beside) + ends))

    def piece(src, k, t, h, send_sem, device):
        return remote(src, blocks.at[k, t, h], send_sem, recv.at[k, h], device)

    def arrived(k, h):
        piece(blocks.at[k, core, h], k, core, h, mate_send, mate).wait_recv()

    def late(k, h):
        return mate_recv.at[k if h == 0 else nrow + k % CORES]

    def to_mate(part, arrival):
        return remote(part, part, mate_send, arrival, mate)

    def mate_got(k):
        to_mate(blocks.at[k, 1 - core], mate_recv.at[k]).wait_recv()

    def left_out(source, move, t, h):
        part = left.at[at(*source), t, h]
        arrival = left_recv.at[at(*source), t, h]
        return remote(part, part, left_send, arrival, (row, at(*move)))

    def left_relay(halves):
        for h in halves:
            for d, t in firsts:
                for move in along_y if t < half else along_x:
                    left_out(d, move, t, h).start()

    def left_rest():
        for d, t in seconds:
            for h in range(SPLIT):
                left_out((0, 0), d, t, h).start()

    def aid_up(d, t, h):
        part, arrival = left.at[at(*d), t, h], aid_recv.at[at(*d), t, h]
        return remote(part, aid.at[at(*d), t, h], aid_send, arrival, (inner_row, col))

    def aid_out(halves):
        for h in halves:
            for c in range(CORES):
                part = blocks.at[end_row - core + c, core, h]
                for d in beside:
                    device = (z * CORES + c, at(*d))
                    arrival = aid_recv.at[col, core, h]
                    remote(part, aid.at[col, core, h], aid_send, arrival, device).start()

    def aid_wait(sources, h):
        for d in sources:
            for t in range(tiles):
                part = aid.at[at(*d), t, h]
                remote(part, part, aid_send, aid_recv.at[at(*d), t, h], mate).wait_recv()

    own_to_mate = remote(left.at[col], blocks.at[row], mate_send, mate_recv.at[row], mate)

    def flags_up(device):
        return remote(flags, aid_flags, flag_sem.at[0], flag_sem.at[1], device)

    def own_up(t, h):
        @pl.when(has_above)
        def _():
            device = ((z + 1) * CORES + t, col)
            piece(left.at[col, t, h], row, t, h, z_send.at[0], device).start()

    def own_down(t, h):
        @pl.when(has_below)
        def _():
            device = ((z - 1) * CORES + t, col)
            piece(left.at[col, t, h], row, t, h, z_send.at[1], device).start()

    low = z < top - z
    for h in range(SPLIT):
        for t in range(tiles):

            @pl.when(low)
            def _():
                own_down(t, h)

            own_up(t, h)

            @pl.when(jnp.logical_not(low))
            def _():
                own_down(t, h)

        if h == 0:
            for d, t in firsts:
                for g in range(SPLIT):
                    left_out((0, 0), d, t, g).start()

            @pl.when(is_inside)
            def _():
                left_rest()

    own_to_mate.start()

    @pl.when(is_end)
    def _():
        flags_up((inner_row, col)).start()

    acc[...] = jnp.zeros_like(acc)
    aid_acc[...] = jnp.zeros_like(aid_acc)

    def square(part):
        return part.reshape(-1, width)

    def multiply(*terms):
        for t in range(tiles):
            acc[t] += sum(
                jnp.dot(
                    square(left[c, i]), square(blocks[k, t]), preferred_element_type=jnp.float32
                )
                for k, c, i in terms
            )

    def multiply_piece(k, t, h):
        a = left[k % ncol, k // ncol, :, :, pl.ds(h * depth, depth)]
        acc[t] += jnp.dot(
            a.reshape(width, depth), blocks[k, t, h], preferred_element_type=jnp.float32
        )

    def from_own(k):
        multiply((k, k % ncol, k // ncol))

    def is_direct(k):
        c = k % ncol
        return (c // nx == y) | (c % nx == x)

    def planes_at(distance, body):
        for sign in (-1, 1) if distance else (1,):
            plane = z + sign * distance
            pl.when((plane >= 0) & (plane < planes))(functools.partial(body, plane))

    def direct_products(distance):
        def run(plane):
            for c in range(CORES):
                k = plane * CORES + c
                if distance:
                    mate_got(k)

                @pl.when(is_direct(k))
                def _():
                    from_own(k)

        planes_at(distance, run)

    def mate_own_got():
        remote(left.at[col], blocks.at[mate_row], mate_send, mate_recv.at[mate_row], mate).wait_recv()

    fillers = []

    def first_filler():
        mate_own_got()
        direct_products(0)

    if planes > 3:
        fillers.append(first_filler)
        for distance in range(1, planes - 2):
            fillers.append(functools.partial(direct_products, distance))

    def relay(step):
        for h in range(SPLIT):
            if step == 1 and h == SPLIT - 1:
                for g in range(SPLIT):
                    for d, t in firsts:
                        left_out(d, d, t, g).wait_recv()
                    if g < SPLIT // 2:
                        left_relay([g])
                    else:
                        pl.when(jnp.logical_not(is_aide))(functools.partial(left_relay, [g]))
                pl.when(is_end)(left_rest)

            for c in range(CORES):
                if step == planes - 2:
                    number = SPLIT * CORES - (h * CORES + c)
                    for _ in range(-(-len(fillers) // number)):
                        pl.when(is_inside)(fillers.pop(0))
                for sign in (-1, 1):
                    plane = z + sign * step

                    @pl.when(is_inside & (plane >= 0) & (plane < planes))
                    def _():
                        k = plane * CORES + c
                        part = blocks.at[k, core, h]
                        arrived(k, h)
                        if sign < 0:
                            piece(part, k, core, h, z_send.at[0], above).start()
                        else:
                            piece(part, k, core, h, z_send.at[1], below).start()
                        to_mate(part, mate_recv.at[k]).start()

    for step in range(1, planes - 1):
        relay(step)
        if step == 1:

            @pl.when(is_aide)
            def _():
                aid_out(range(SPLIT // 2))
                left_relay(range(SPLIT // 2, SPLIT))
                aid_out(range(SPLIT // 2, SPLIT))

            @pl.when(is_end)
            def _():
                for h in range(SPLIT):
                    for t in range(tiles):
                        for d in across:
                            left_out(d, d, t, h).wait_recv()
                            aid_up(d, t, h).start()

            for d, t in seconds:
                for h in range(SPLIT):
                    left_out(d, d, t, h).wait_recv()

    def to_row(slot, d):
        part = sums.at[slot]
        return remote(part, part, sum_sem.at[0], sum_sem.at[1], ((row + d) % nrow, col))

    def some_sums(number):
        part = sums.at[pl.ds(0, number)]
        return remote(part, part, sum_sem.at[0], sum_sem.at[1], mate)

    def send_sums(slot, values, weights):
        for t in range(tiles):
            sums[slot, t] = jnp.sum(values[t] * values[t], axis=0) * weights[t]
        for d in range(1, nrow):
            to_row(slot, d).start()

    def aid_own():
        for t in range(tiles):
            k = col + ncol * t
            for i in range(tiles):
                aid_acc[i] += jnp.dot(
                    square(blocks[end_row, t]), square(blocks[k, i]),
                    preferred_element_type=jnp.float32,
                )

    def aid_multiply(sources, h):
        aid_wait(sources, h)
        if sources:
            for i in range(tiles):
                aid_acc[i, pl.ds(h * depth, depth)] += sum(
                    jnp.dot(
                        aid[at(*d), t, h], square(blocks[at(*d) + ncol * t, i]),
                        preferred_element_type=jnp.float32,
                    )
                    for d in sources
                    for t in range(tiles)
                )

    def inside():
        direct_products(planes - 2)

        @pl.when(is_aide)
        def _():
            aid_own()
            for h in range(SPLIT // 2):
                aid_multiply(beside + across, h)
            for h in range(SPLIT // 2, SPLIT):
                aid_multiply(across, h)

        for d in across:
            for t in range(tiles):
                for h in range(SPLIT):
                    left_out(d, d, t, h).wait_recv()
        if across:
            multiply(*((at(*d) + ncol * t, at(*d), t) for d in across for t in range(tiles)))
        send_sums(row, acc, flags)

        @pl.when(is_aide)
        def _():
            for h in range(SPLIT // 2, SPLIT):
                aid_multiply(beside, h)
            flags_up(mate).wait_recv()
            send_sums(end_row, aid_acc, aid_flags)

    def outside():
        mate_own_got()

        def near(plane):
            for c in range(CORES):
                from_own(plane * CORES + c)

        planes_at(0, near)

        def nearer(plane):
            for h in range(SPLIT):
                for c in range(CORES):
                    k = plane * CORES + c
                    arrived(k, h)
                    to_mate(blocks.at[k, core, h], mate_recv.at[k]).start()
            for c in range(CORES):
                mate_got(plane * CORES + c)
                from_own(plane * CORES + c)

        for distance in range(1, top):
            planes_at(distance, nearer)

        def farthest(plane):
            for h in range(SPLIT):
                for c in range(CORES):
                    k = plane * CORES + c
                    arrived(k, h)
                    to_mate(blocks.at[k, core, h], late(k, h)).start()
                    multiply_piece(k, core, h)
            for h in range(SPLIT):
                for c in range(CORES):
                    k = plane * CORES + c
                    to_mate(blocks.at[k, 1 - core, h], late(k, h)).wait_recv()
                    multiply_piece(k, 1 - core, h)

        planes_at(top, farthest)

    pl.when(is_inside)(inside)
    pl.when(is_end)(outside)

    @pl.when(is_end)
    def _():
        some_sums(nrow).wait_recv()

    @pl.when(is_aide)
    def _():
        some_sums(nrow - 2).wait_recv()

    if planes > 4:

        @pl.when(jnp.logical_not(is_end | is_aide))
        def _():
            some_sums(nrow - 1).wait_recv()

    for s in range(tiles):
        out = jnp.zeros((width, width), jnp.float32)
        held = jnp.float32(0)
        for t in range(tiles):
            w = (cols[0, s] == col + ncol * t).astype(jnp.float32)
            held = held + w
            total = sums[0, t]
            for k in range(1, nrow):
                total = total + sums[k, t]
            safe = jnp.where(total > 0, total, 1.0)
            scale = jnp.float32(0.5 * nrow * width) / safe * w
            out = out + acc[t] * acc[t] * scale[None, :]
        out_ref[0, s] = out + raw[s].astype(jnp.float32) * (0.5 * held)

    def sent(part, sem):
        remote(part, part, sem, sem, mate).wait_send()

    for p in range(planes):

        @pl.when(z == p)
        def _():
            if p < top:
                sent(blocks.at[pl.ds(0, (p + 1) * CORES), 0], z_send.at[0])
            if p > 0:
                sent(blocks.at[pl.ds(0, (planes - p) * CORES), 0], z_send.at[1])

    sent(blocks.at[:, 0], mate_send)
    sent(left.at[pl.ds(0, ncol - 1)], left_send)

    @pl.when(is_end)
    def _():
        if across:
            sent(aid.at[pl.ds(0, len(across))], aid_send)
        flags_up(mate).wait_send()

    @pl.when(is_inside)
    def _():
        some_sums(nrow - 1).wait_send()

    @pl.when(is_aide)
    def _():
        some_sums(nrow - 1).wait_send()
        sent(aid.at[pl.ds(0, len(beside))], aid_send)


def on_device(nrow, ncol, flow_tiles, tile_cols, pairs):
    _, tiles, _, width = flow_tiles.shape
    depth = width // SPLIT
    dma = pltpu.SemaphoreType.DMA
    return pl.pallas_call(
        functools.partial(kernel, nrow, ncol),
        out_shape=jax.ShapeDtypeStruct(flow_tiles.shape, jnp.float32),
        in_specs=[pl.BlockSpec(memory_space=pltpu.HBM)] * 2,
        out_specs=pl.BlockSpec(memory_space=pltpu.VMEM),
        scratch_shapes=[
            pltpu.SMEM((1, tiles), jnp.int32),
            pltpu.VMEM((tiles, width, width), jnp.bfloat16),
            pltpu.VMEM((ncol, tiles, SPLIT, depth, width), jnp.bfloat16),
            pltpu.VMEM((nrow, tiles, SPLIT, depth, width), jnp.bfloat16),
            pltpu.VMEM((ncol, tiles, SPLIT, depth, width), jnp.bfloat16),
            pltpu.VMEM((tiles, width, width), jnp.float32),
            pltpu.VMEM((tiles, width, width), jnp.float32),
            pltpu.VMEM((tiles, width), jnp.float32),
            pltpu.VMEM((tiles, width), jnp.float32),
            pltpu.VMEM((nrow, tiles, width), jnp.float32),
            dma((2,)),
            dma((2,)),
            dma,
            dma((nrow, SPLIT)),
            dma((nrow + CORES,)),
            dma,
            dma((ncol, tiles, SPLIT)),
            dma,
            dma((ncol, tiles, SPLIT)),
            dma((2,)),
            dma((2,)),
        ],
        compiler_params=pltpu.CompilerParams(
            collective_id=0, has_side_effects=True, vmem_limit_bytes=24 * 1024 * 1024
        ),
        name="cluster_step",
    )(
        pltpu.with_memory_space_constraint(tile_cols, pltpu.HBM),
        pltpu.with_memory_space_constraint(flow_tiles, pltpu.HBM),
    )


def solution(mesh):
    placed = (P("row", "col", None, None), P("row", "col"), P(("row", "col"), None))
    return jax.shard_map(
        functools.partial(on_device, mesh.shape["row"], mesh.shape["col"]),
        mesh=mesh,
        in_specs=placed,
        out_specs=P("row", "col", None, None),
        check_vma=False,
    )
```

```python
import functools
import math

import jax
import jax.numpy as jnp
from jax import lax
from jax.experimental import pallas as pl
from jax.experimental.pallas import tpu as pltpu
from jax.sharding import PartitionSpec as P

MESH = pl.DeviceIdType.MESH
CORES = 2
SPLIT = 2


def remote(src, dst, send_sem, recv_sem, device):
    return pltpu.make_async_remote_copy(
        src_ref=src,
        dst_ref=dst,
        send_sem=send_sem,
        recv_sem=recv_sem,
        device_id=device,
        device_id_type=MESH,
    )


def kernel(
    nrow, ncol, cols_hbm, flow_hbm, out_ref,
    cols, raw, left, blocks, aid, acc, aid_acc, flags, aid_flags, sums,
    in_sem, z_send, mate_send, recv, mate_recv, left_send, left_recv,
    aid_send, aid_recv, flag_sem, sum_sem,
):
    tiles, width = raw.shape[0], raw.shape[2]
    depth = left.shape[3]
    planes = nrow // CORES
    row, col = lax.axis_index("row"), lax.axis_index("col")
    z, core = row // CORES, row % CORES
    mate_row = row + 1 - 2 * core
    mate = (mate_row, col)
    above, below = (row + CORES, col), (row - CORES, col)
    has_above, has_below = z < planes - 1, z > 0
    ny = math.isqrt(ncol)
    ny = ny if ny * ny == ncol else 1
    nx = ncol // ny
    y, x = col // nx, col % nx
    half = tiles // 2
    top = planes - 1
    is_end = (z == 0) | (z == top)
    is_inside = jnp.logical_not(is_end)
    is_aide = (z == 1) | (z == top - 1)
    end_row = jnp.where(z <= 1, 0, top) * CORES + core
    inner_row = jnp.where(z == 0, 1, top - 1) * CORES + core

    def at(dy, dx):
        return ((y + dy) % ny) * nx + (x + dx) % nx

    along_x = [(0, dx) for dx in range(1, nx)]
    along_y = [(dy, 0) for dy in range(1, ny)]
    beside = along_x + along_y
    across = [(dy, dx) for dy, _ in along_y for _, dx in along_x]
    firsts = [(d, t) for t in range(half) for d in along_x]
    firsts += [(d, t) for t in range(half, tiles) for d in along_y]
    seconds = [(d, t) for t in range(half, tiles) for d in along_x]
    seconds += [(d, t) for t in range(half) for d in along_y]
    topped = nx == ny and tiles == CORES
    kept = depth // 4

    load_cols = pltpu.make_async_copy(cols_hbm, cols, in_sem.at[0])
    load_flow = pltpu.make_async_copy(flow_hbm.at[0], raw, in_sem.at[1])
    load_cols.start()
    load_flow.start()

    barrier = pltpu.get_barrier_semaphore()

    def greet(device):
        pl.semaphore_signal(barrier, inc=1, device_id=device, device_id_type=MESH)

    greet(mate)
    for d in beside:
        greet((row, at(*d)))
        greet((mate_row, at(*d)))

    @pl.when(has_above)
    def _():
        for c in range(CORES):
            greet(((z + 1) * CORES + c, col))

    @pl.when(has_below)
    def _():
        for c in range(CORES):
            greet(((z - 1) * CORES + c, col))

    load_cols.wait()
    load_flow.wait()
    for t in range(tiles):
        target = col + ncol * t
        tile = jnp.zeros((width, width), jnp.float32)
        weight = jnp.float32(0)
        for s in range(tiles):
            w = (cols[0, s] == target).astype(jnp.float32)
            weight = weight + w
            tile = tile + raw[s].astype(jnp.float32) * w
        flags[t] = jnp.full((width,), weight, jnp.float32)
        tile = tile.astype(jnp.bfloat16).reshape(SPLIT, depth, width)
        left[col, t] = tile
        blocks[row, t] = tile

    ends = jnp.where(has_above, 1, 0) + jnp.where(has_below, 1, 0)
    pl.semaphore_wait(barrier, 1 + CORES * (len(beside) + ends))

    def piece(src, k, t, h, up, device):
        index = k if up else k - CORES
        send_sem = z_send.at[0 if up else 1]
        return remote(src, blocks.at[k, t, h], send_sem, recv.at[index, h], device)

    def arrived(k, h, up):
        piece(blocks.at[k, core, h], k, core, h, up, mate).wait_recv()

    def to_mate(part, arrival):
        return remote(part, part, mate_send, arrival, mate)

    def mate_got(plane):
        part = blocks.at[pl.ds(plane * CORES, CORES), 1 - core]
        to_mate(part, mate_recv.at[plane]).wait_recv()

    def late(plane, h):
        return mate_recv.at[plane if h == 0 else top + h]

    def got(part, sem):
        remote(part, part, sem, sem, mate).wait_recv()

    def left_out(source, move, t, h):
        part = left.at[at(*source), t, h]
        if source != (0, 0):
            kind = SPLIT + h
        else:
            kind = h if (move, t) in firsts else 2 * SPLIT
        return remote(part, part, left_send, left_recv.at[kind], (row, at(*move)))

    def first_got(h):
        got(left.at[pl.ds(0, len(firsts)), 0, 0], left_recv.at[h])

    def second_got():
        got(left.at[pl.ds(0, len(seconds)), 0], left_recv.at[2 * SPLIT])

    def across_got(h):
        got(left.at[pl.ds(0, len(across)), :, 0], left_recv.at[SPLIT + h])

    def left_relay(halves):
        for h in halves:
            for d, t in firsts:
                for move in along_y if t < half else along_x:
                    left_out(d, move, t, h).start()

    def left_rest():
        for d, t in seconds:
            for h in range(SPLIT):
                left_out((0, 0), d, t, h).start()

    def aid_up(d, t, h):
        part = left.at[at(*d), t, h]
        arrival = aid_recv.at[SPLIT + h]
        return remote(part, aid.at[at(*d), t, h], aid_send.at[0], arrival, (inner_row, col))

    def top_up():
        for d, t in firsts:
            part = left.at[at(*d), t, SPLIT - 1, pl.ds(kept, depth - kept)]
            target = aid.at[at(*d), t, SPLIT - 1, pl.ds(kept, depth - kept)]
            arrival = aid_recv.at[2 * SPLIT]
            remote(part, target, aid_send.at[1], arrival, (inner_row, col)).start()

    def aid_out(halves):
        def send(h, c, sources, number=depth, sem=aid_send.at[0], arrival=None):
            part = blocks.at[end_row - core + c, core, h, pl.ds(0, number)]
            target = aid.at[col, core, h, pl.ds(0, number)]
            for d in sources:
                device = (z * CORES + c, at(*d))
                remote(part, target, sem, arrival or aid_recv.at[h], device).start()

        def send_late(h, c, by_top, others):
            send(h, c, others)
            send(h, c, by_top, kept, aid_send.at[2], aid_recv.at[2 * SPLIT + 1])

        for h in halves:
            for c in range(CORES):
                if topped and h == SPLIT - 1:
                    pl.when(core < half)(functools.partial(send_late, h, c, along_x, along_y))
                    pl.when(core >= half)(functools.partial(send_late, h, c, along_y, along_x))
                else:
                    send(h, c, beside)

    by_top = aid.at[pl.ds(0, len(beside)), 0, 0, pl.ds(kept, depth - kept)]
    not_by_top = aid.at[pl.ds(0, len(beside)), 0, 0, pl.ds(0, kept)]

    def aid_beside_got(h):
        if topped and h == SPLIT - 1:
            got(by_top, aid_recv.at[2 * SPLIT])
            got(aid.at[pl.ds(0, len(beside)), 0, 0], aid_recv.at[h])
            got(not_by_top, aid_recv.at[2 * SPLIT + 1])
        else:
            got(aid.at[pl.ds(0, len(beside)), :, 0], aid_recv.at[h])

    def aid_across_got(h):
        if across:
            got(aid.at[pl.ds(0, len(across)), :, 0], aid_recv.at[SPLIT + h])

    own_to_mate = remote(left.at[col], blocks.at[row], mate_send, mate_recv.at[z], mate)

    def flags_up(device):
        return remote(flags, aid_flags, flag_sem.at[0], flag_sem.at[1], device)

    def own_up(t, h):
        @pl.when(has_above)
        def _():
            device = ((z + 1) * CORES + t, col)
            piece(left.at[col, t, h], row, t, h, True, device).start()

    def own_down(t, h):
        @pl.when(has_below)
        def _():
            device = ((z - 1) * CORES + t, col)
            piece(left.at[col, t, h], row, t, h, False, device).start()

    low = z < top - z
    for h in range(SPLIT):
        for t in range(tiles):

            @pl.when(low)
            def _():
                own_down(t, h)

            own_up(t, h)

            @pl.when(jnp.logical_not(low))
            def _():
                own_down(t, h)

        if h == 0:
            for d, t in firsts:
                for g in range(SPLIT):
                    left_out((0, 0), d, t, g).start()

            @pl.when(is_inside)
            def _():
                left_rest()

    own_to_mate.start()

    @pl.when(is_end)
    def _():
        flags_up((inner_row, col)).start()

    acc[...] = jnp.zeros_like(acc)
    aid_acc[...] = jnp.zeros_like(aid_acc)

    def square(part):
        return part.reshape(-1, width)

    def multiply(*terms):
        for t in range(tiles):
            acc[t] += sum(
                jnp.dot(
                    square(left[c, i]), square(blocks[k, t]), preferred_element_type=jnp.float32
                )
                for k, c, i in terms
            )

    def multiply_piece(k, t, h):
        a = left[k % ncol, k // ncol, :, :, pl.ds(h * depth, depth)]
        acc[t] += jnp.dot(
            a.reshape(width, depth), blocks[k, t, h], preferred_element_type=jnp.float32
        )

    def from_own(k):
        multiply((k, k % ncol, k // ncol))

    def is_direct(k):
        c = k % ncol
        return (c // nx == y) | (c % nx == x)

    def planes_at(distance, body):
        for sign in (-1, 1) if distance else (1,):
            plane = z + sign * distance
            pl.when((plane >= 0) & (plane < planes))(functools.partial(body, plane))

    def direct_products(distance):
        def run(plane):
            if distance:
                mate_got(plane)
            for c in range(CORES):
                k = plane * CORES + c

                @pl.when(is_direct(k))
                def _():
                    from_own(k)

        planes_at(distance, run)

    def mate_own_got():
        got(blocks.at[mate_row], mate_recv.at[z])

    fillers = []

    def first_filler():
        mate_own_got()
        direct_products(0)

    if planes > 3:
        fillers.append(first_filler)
        for distance in range(1, planes - 2):
            fillers.append(functools.partial(direct_products, distance))

    def relay(step):
        for h in range(SPLIT):
            if step == 1 and h == SPLIT - 1:
                for g in range(SPLIT):
                    first_got(g)
                    if g < SPLIT // 2:
                        left_relay([g])
                    else:
                        pl.when(jnp.logical_not(is_aide))(functools.partial(left_relay, [g]))
                if topped:
                    pl.when(is_end)(top_up)
                pl.when(is_end)(left_rest)

            for c in range(CORES):
                if step == planes - 2:
                    number = SPLIT * CORES - (h * CORES + c)
                    for _ in range(-(-len(fillers) // number)):
                        pl.when(is_inside)(fillers.pop(0))
                for sign in (-1, 1):
                    plane = z + sign * step

                    @pl.when(is_inside & (plane >= 0) & (plane < planes))
                    def _():
                        k = plane * CORES + c
                        part = blocks.at[k, core, h]
                        arrived(k, h, sign < 0)
                        piece(part, k, core, h, sign < 0, above if sign < 0 else below).start()
                        to_mate(part, mate_recv.at[plane]).start()

    for step in range(1, planes - 1):
        relay(step)
        if step == 1:

            @pl.when(is_aide)
            def _():
                aid_out(range(SPLIT // 2))
                left_relay(range(SPLIT // 2, SPLIT))
                aid_out(range(SPLIT // 2, SPLIT))

            @pl.when(is_end)
            def _():
                for h in range(SPLIT):
                    if across:
                        across_got(h)
                    for t in range(tiles):
                        for d in across:
                            aid_up(d, t, h).start()

            second_got()

    def to_row(slot, d):
        part = sums.at[slot]
        device = ((row + jnp.where(low, d, nrow - d)) % nrow, col)
        return remote(part, part, sum_sem.at[0], sum_sem.at[1], device)

    def some_sums(number):
        part = sums.at[pl.ds(0, number)]
        return remote(part, part, sum_sem.at[0], sum_sem.at[1], mate)

    def send_sums(slot, values, weights):
        for t in range(tiles):
            sums[slot, t] = jnp.sum(values[t] * values[t], axis=0) * weights[t]
        for d in range(1, nrow):
            to_row(slot, d).start()

    def aid_own():
        for t in range(tiles):
            k = col + ncol * t
            for i in range(tiles):
                aid_acc[i] += jnp.dot(
                    square(blocks[end_row, t]), square(blocks[k, i]),
                    preferred_element_type=jnp.float32,
                )

    def aid_multiply(sources, h):
        if sources:
            for i in range(tiles):
                aid_acc[i, pl.ds(h * depth, depth)] += sum(
                    jnp.dot(
                        aid[at(*d), t, h], square(blocks[at(*d) + ncol * t, i]),
                        preferred_element_type=jnp.float32,
                    )
                    for d in sources
                    for t in range(tiles)
                )

    def inside():
        direct_products(planes - 2)

        @pl.when(is_aide)
        def _():
            aid_own()
            for h in range(SPLIT // 2):
                aid_beside_got(h)
                aid_multiply(beside, h)
            for h in range(SPLIT // 2):
                aid_across_got(h)
                aid_multiply(across, h)

        if across:
            for h in range(SPLIT):
                across_got(h)
            multiply(*((at(*d) + ncol * t, at(*d), t) for d in across for t in range(tiles)))
        send_sums(row, acc, flags)

        @pl.when(is_aide)
        def _():
            for h in range(SPLIT // 2, SPLIT):
                aid_beside_got(h)
                aid_multiply(beside, h)
                aid_across_got(h)
                aid_multiply(across, h)
            flags_up(mate).wait_recv()
            send_sums(end_row, aid_acc, aid_flags)

    def outside():
        mate_own_got()

        def near(plane):
            for c in range(CORES):
                from_own(plane * CORES + c)

        planes_at(0, near)

        def nearer(up, plane):
            for h in range(SPLIT):
                for c in range(CORES):
                    k = plane * CORES + c
                    arrived(k, h, up)
                    to_mate(blocks.at[k, core, h], mate_recv.at[plane]).start()
            mate_got(plane)
            for c in range(CORES):
                from_own(plane * CORES + c)

        def farthest(up, plane):
            for h in range(SPLIT):
                for c in range(CORES):
                    k = plane * CORES + c
                    arrived(k, h, up)
                    to_mate(blocks.at[k, core, h], late(plane, h)).start()
                    multiply_piece(k, core, h)
            for h in range(SPLIT):
                got(blocks.at[pl.ds(plane * CORES, CORES), 1 - core, h], late(plane, h))
                for c in range(CORES):
                    multiply_piece(plane * CORES + c, 1 - core, h)

        for distance in range(1, planes):
            body = nearer if distance < top else farthest
            pl.when(z == 0)(functools.partial(body, False, distance))
            pl.when(z == top)(functools.partial(body, True, top - distance))

    pl.when(is_inside)(inside)
    pl.when(is_end)(outside)

    @pl.when(is_end)
    def _():
        some_sums(nrow).wait_recv()

    @pl.when(is_aide)
    def _():
        some_sums(nrow - 2).wait_recv()

    if planes > 4:

        @pl.when(jnp.logical_not(is_end | is_aide))
        def _():
            some_sums(nrow - 1).wait_recv()

    for s in range(tiles):
        held, slot = jnp.float32(0), jnp.int32(0)
        for t in range(tiles):
            match = cols[0, s] == col + ncol * t
            held = held + match.astype(jnp.float32)
            slot = slot + match.astype(jnp.int32) * t
        total = jnp.zeros((width,), jnp.float32)
        for t in range(tiles):
            part = sums[0, t]
            for k in range(1, nrow):
                part = part + sums[k, t]
            total = total + part * (slot == t).astype(jnp.float32)
        safe = jnp.where(total > 0, total, 1.0)
        scale = jnp.float32(0.5 * nrow * width) / safe * held
        value = acc[slot]
        out_ref[0, s] = value * value * scale[None, :] + raw[s].astype(jnp.float32) * (0.5 * held)

    def sent(part, sem):
        remote(part, part, sem, sem, mate).wait_send()

    for p in range(planes):

        @pl.when(z == p)
        def _():
            if p < top:
                sent(blocks.at[pl.ds(0, (p + 1) * CORES), 0], z_send.at[0])
            if p > 0:
                sent(blocks.at[pl.ds(0, (planes - p) * CORES), 0], z_send.at[1])

    sent(blocks.at[:, 0], mate_send)
    sent(left.at[pl.ds(0, ncol - 1)], left_send)

    @pl.when(is_end)
    def _():
        if across:
            sent(blocks.at[pl.ds(0, len(across) * tiles), 0], aid_send.at[0])
        if topped:
            sent(by_top, aid_send.at[1])
        flags_up(mate).wait_send()

    @pl.when(is_inside)
    def _():
        some_sums(nrow - 1).wait_send()

    @pl.when(is_aide)
    def _():
        some_sums(nrow - 1).wait_send()
        if topped:
            sent(blocks.at[pl.ds(0, 3 * len(along_x)), 0], aid_send.at[0])
            sent(not_by_top, aid_send.at[2])
        else:
            sent(blocks.at[pl.ds(0, len(beside) * CORES), 0], aid_send.at[0])


def on_device(nrow, ncol, flow_tiles, tile_cols, pairs):
    _, tiles, _, width = flow_tiles.shape
    depth = width // SPLIT
    dma = pltpu.SemaphoreType.DMA
    return pl.pallas_call(
        functools.partial(kernel, nrow, ncol),
        out_shape=jax.ShapeDtypeStruct(flow_tiles.shape, jnp.float32),
        in_specs=[pl.BlockSpec(memory_space=pltpu.HBM)] * 2,
        out_specs=pl.BlockSpec(memory_space=pltpu.VMEM),
        scratch_shapes=[
            pltpu.SMEM((1, tiles), jnp.int32),
            pltpu.VMEM((tiles, width, width), jnp.bfloat16),
            pltpu.VMEM((ncol, tiles, SPLIT, depth, width), jnp.bfloat16),
            pltpu.VMEM((nrow, tiles, SPLIT, depth, width), jnp.bfloat16),
            pltpu.VMEM((ncol, tiles, SPLIT, depth, width), jnp.bfloat16),
            pltpu.VMEM((tiles, width, width), jnp.float32),
            pltpu.VMEM((tiles, width, width), jnp.float32),
            pltpu.VMEM((tiles, width), jnp.float32),
            pltpu.VMEM((tiles, width), jnp.float32),
            pltpu.VMEM((nrow, tiles, width), jnp.float32),
            dma((2,)),
            dma((2,)),
            dma,
            dma((nrow - CORES, SPLIT)),
            dma((nrow // CORES + SPLIT - 1,)),
            dma,
            dma((2 * SPLIT + 1,)),
            dma((3,)),
            dma((2 * SPLIT + 2,)),
            dma((2,)),
            dma((2,)),
        ],
        compiler_params=pltpu.CompilerParams(
            collective_id=0, has_side_effects=True, vmem_limit_bytes=24 * 1024 * 1024
        ),
        name="cluster_step",
    )(
        pltpu.with_memory_space_constraint(tile_cols, pltpu.HBM),
        pltpu.with_memory_space_constraint(flow_tiles, pltpu.HBM),
    )


def solution(mesh):
    placed = (P("row", "col", None, None), P("row", "col"), P(("row", "col"), None))
    return jax.shard_map(
        functools.partial(on_device, mesh.shape["row"], mesh.shape["col"]),
        mesh=mesh,
        in_specs=placed,
        out_specs=P("row", "col", None, None),
        check_vma=False,
    )
```

```python
import functools
import math

import jax
import jax.numpy as jnp
from jax import lax
from jax.experimental import pallas as pl
from jax.experimental.pallas import tpu as pltpu
from jax.sharding import PartitionSpec as P

MESH = pl.DeviceIdType.MESH
CORES = 2
SPLIT = 2


def remote(src, dst, send_sem, recv_sem, device):
    return pltpu.make_async_remote_copy(
        src_ref=src,
        dst_ref=dst,
        send_sem=send_sem,
        recv_sem=recv_sem,
        device_id=device,
        device_id_type=MESH,
    )


def kernel(
    nrow, ncol, cols_hbm, flow_hbm, out_ref,
    cols, raw, left, blocks, aid, acc, aid_acc, flags, aid_flags, sums,
    z_send, mate_send, recv, mate_recv, left_send, left_recv,
    aid_send, aid_recv, sum_sem, last_sem,
):
    tiles, width = raw.shape[0], raw.shape[2]
    depth = left.shape[3]
    planes = nrow // CORES
    row, col = lax.axis_index("row"), lax.axis_index("col")
    z, core = row // CORES, row % CORES
    mate_row = row + 1 - 2 * core
    mate = (mate_row, col)
    above, below = (row + CORES, col), (row - CORES, col)
    has_above, has_below = z < planes - 1, z > 0
    ny = math.isqrt(ncol)
    ny = ny if ny * ny == ncol else 1
    nx = ncol // ny
    y, x = col // nx, col % nx
    half = tiles // 2
    top = planes - 1
    is_end = (z == 0) | (z == top)
    is_inside = jnp.logical_not(is_end)
    is_aide = (z == 1) | (z == top - 1)
    end_row = jnp.where(z <= 1, 0, top) * CORES + core
    inner_row = jnp.where(z == 0, 1, top - 1) * CORES + core

    def at(dy, dx):
        return ((y + dy) % ny) * nx + (x + dx) % nx

    along_x = [(0, dx) for dx in range(1, nx)]
    along_y = [(dy, 0) for dy in range(1, ny)]
    beside = along_x + along_y
    across = [(dy, dx) for dy, _ in along_y for _, dx in along_x]
    firsts = [(d, t) for t in range(half) for d in along_x]
    firsts += [(d, t) for t in range(half, tiles) for d in along_y]
    seconds = [(d, t) for t in range(half, tiles) for d in along_x]
    seconds += [(d, t) for t in range(half) for d in along_y]
    topped = nx == ny and tiles == CORES
    kept = depth // 4
    spare = kept

    load_cols = pltpu.make_async_copy(cols_hbm, cols, left_send)
    load_flow = pltpu.make_async_copy(flow_hbm.at[0], raw, mate_send)
    load_cols.start()
    load_flow.start()

    barrier = pltpu.get_barrier_semaphore()

    def greet(device):
        pl.semaphore_signal(barrier, inc=1, device_id=device, device_id_type=MESH)

    greet(mate)
    for d in beside:
        greet((row, at(*d)))
        greet((mate_row, at(*d)))

    @pl.when(has_above)
    def _():
        for c in range(CORES):
            greet(((z + 1) * CORES + c, col))

    @pl.when(has_below)
    def _():
        for c in range(CORES):
            greet(((z - 1) * CORES + c, col))

    load_cols.wait()
    load_flow.wait()
    for t in range(tiles):
        target = col + ncol * t
        tile = jnp.zeros((width, width), jnp.float32)
        weight = jnp.float32(0)
        for s in range(tiles):
            w = (cols[0, s] == target).astype(jnp.float32)
            weight = weight + w
            tile = tile + raw[s].astype(jnp.float32) * w
        flags[t] = jnp.full((width,), weight, jnp.float32)
        tile = tile.astype(jnp.bfloat16).reshape(SPLIT, depth, width)
        left[col, t] = tile
        blocks[row, t] = tile

    ends = jnp.where(has_above, 1, 0) + jnp.where(has_below, 1, 0)
    pl.semaphore_wait(barrier, 1 + CORES * (len(beside) + ends))

    def piece(src, k, t, h, up, device):
        index = k if up else k - CORES
        send_sem = z_send
        return remote(src, blocks.at[k, t, h], send_sem, recv.at[index, h], device)

    def arrived(k, h, up):
        piece(blocks.at[k, core, h], k, core, h, up, mate).wait_recv()

    def last_piece(k, up, device):
        send_sem = z_send
        body, rest = last_body(k, core), last_rest(k, core)
        index = k if up else k - CORES
        remote(body, body, send_sem, recv.at[index, SPLIT - 1], device).start()
        remote(rest, rest, send_sem, last_sem.at[0], device).start()
        other = (device[0] + 1 - 2 * core, col)
        remote(rest, rest, aid_send.at[1], last_sem.at[1], other).start()

    def last_body(k, t):
        return blocks.at[k, t, SPLIT - 1, pl.ds(0, depth - spare)]

    def last_rest(k, t):
        return blocks.at[k, t, SPLIT - 1, pl.ds(depth - spare, spare)]

    def to_mate(part, arrival, sem=mate_send):
        return remote(part, part, sem, arrival, mate)

    def mate_got(plane):
        part = blocks.at[pl.ds(plane * CORES, CORES), 1 - core]
        to_mate(part, mate_recv.at[plane]).wait_recv()

    def late(plane, h, c):
        return mate_recv.at[plane if h == 0 else top + (h - 1) * CORES + c + 1]

    def got(part, sem):
        remote(part, part, sem, sem, mate).wait_recv()

    def left_out(source, move, t, h):
        part = left.at[at(*source), t, h]
        if source != (0, 0):
            kind = SPLIT + h
        else:
            kind = h if (move, t) in firsts else 2 * SPLIT
        return remote(part, part, left_send, left_recv.at[kind], (row, at(*move)))

    def first_got(h):
        got(left.at[pl.ds(0, len(firsts)), 0, 0], left_recv.at[h])

    def second_got():
        got(left.at[pl.ds(0, len(seconds)), 0], left_recv.at[2 * SPLIT])

    def across_got(h):
        got(left.at[pl.ds(0, len(across)), :, 0], left_recv.at[SPLIT + h])

    def left_relay(halves):
        for h in halves:
            for d, t in firsts:
                for move in along_y if t < half else along_x:
                    left_out(d, move, t, h).start()

    def left_rest():
        for d, t in seconds:
            for h in range(SPLIT):
                left_out((0, 0), d, t, h).start()

    def aid_up(d, t, h):
        part = left.at[at(*d), t, h]
        arrival = aid_recv.at[SPLIT + h]
        return remote(part, aid.at[at(*d), t, h], aid_send.at[0], arrival, (inner_row, col))

    def top_up():
        for d, t in firsts:
            part = left.at[at(*d), t, SPLIT - 1, pl.ds(kept, depth - kept)]
            target = aid.at[at(*d), t, SPLIT - 1, pl.ds(kept, depth - kept)]
            arrival = aid_recv.at[SPLIT - 1]
            remote(part, target, aid_send.at[1], arrival, (inner_row, col)).start()

    def aid_out(halves):
        def send(h, c, sources, number=depth, sem=aid_send.at[0]):
            part = blocks.at[end_row - core + c, core, h, pl.ds(0, number)]
            target = aid.at[col, core, h, pl.ds(0, number)]
            for d in sources:
                device = (z * CORES + c, at(*d))
                remote(part, target, sem, aid_recv.at[h], device).start()

        def send_late(h, c, by_top, others):
            send(h, c, others)
            send(h, c, by_top, kept, aid_send.at[1])

        for h in halves:
            for c in range(CORES):
                if topped and h == SPLIT - 1:
                    pl.when(core < half)(functools.partial(send_late, h, c, along_x, along_y))
                    pl.when(core >= half)(functools.partial(send_late, h, c, along_y, along_x))
                else:
                    send(h, c, beside)

    def aid_beside_got(h):
        got(aid.at[pl.ds(0, len(beside)), :, 0], aid_recv.at[h])

    def aid_across_got(h):
        if across:
            got(aid.at[pl.ds(0, len(across)), :, 0], aid_recv.at[SPLIT + h])

    own_to_mate = remote(left.at[col], blocks.at[row], mate_send, mate_recv.at[z], mate)

    def own_up(t, h):
        @pl.when(has_above)
        def _():
            device = ((z + 1) * CORES + t, col)
            piece(left.at[col, t, h], row, t, h, True, device).start()

    def own_down(t, h):
        @pl.when(has_below)
        def _():
            device = ((z - 1) * CORES + t, col)
            piece(left.at[col, t, h], row, t, h, False, device).start()

    low = z < top - z
    for h in range(SPLIT):
        for t in range(tiles):

            @pl.when(low)
            def _():
                own_down(t, h)

            own_up(t, h)

            @pl.when(jnp.logical_not(low))
            def _():
                own_down(t, h)

        if h == 0:
            for d, t in firsts:
                for g in range(SPLIT):
                    left_out((0, 0), d, t, g).start()

            @pl.when(is_inside)
            def _():
                left_rest()

    own_to_mate.start()

    acc[...] = jnp.zeros_like(acc)
    aid_acc[...] = jnp.zeros_like(aid_acc)

    def square(part):
        return part.reshape(-1, width)

    def multiply(*terms):
        for t in range(tiles):
            acc[t] += sum(
                jnp.dot(
                    square(left[c, i]), square(blocks[k, t]), preferred_element_type=jnp.float32
                )
                for k, c, i in terms
            )

    def multiply_piece(k, t, h):
        a = left[k % ncol, k // ncol, :, :, pl.ds(h * depth, depth)]
        acc[t] += jnp.dot(
            a.reshape(width, depth), blocks[k, t, h], preferred_element_type=jnp.float32
        )

    def from_own(k):
        multiply((k, k % ncol, k // ncol))

    def is_direct(k):
        c = k % ncol
        return (c // nx == y) | (c % nx == x)

    def planes_at(distance, body):
        for sign in (-1, 1) if distance else (1,):
            plane = z + sign * distance
            pl.when((plane >= 0) & (plane < planes))(functools.partial(body, plane))

    def direct_products(distance):
        def run(plane):
            if distance:
                mate_got(plane)
            for c in range(CORES):
                k = plane * CORES + c

                @pl.when(is_direct(k))
                def _():
                    from_own(k)

        planes_at(distance, run)

    def mate_own_got():
        got(blocks.at[mate_row], mate_recv.at[z])

    fillers = []

    def first_filler():
        mate_own_got()
        direct_products(0)

    if planes > 3:
        fillers.append(first_filler)
        for distance in range(1, planes - 2):
            fillers.append(functools.partial(direct_products, distance))

    def relay(step):
        for h in range(SPLIT):
            if step == 1 and h == SPLIT - 1:
                for g in range(SPLIT):
                    first_got(g)
                    if g < SPLIT // 2:
                        left_relay([g])
                    else:
                        pl.when(jnp.logical_not(is_aide))(functools.partial(left_relay, [g]))
                if topped:
                    pl.when(is_end)(top_up)
                pl.when(is_end)(left_rest)

            for c in range(CORES):
                if step == planes - 2:
                    number = SPLIT * CORES - (h * CORES + c)
                    for _ in range(-(-len(fillers) // number)):
                        pl.when(is_inside)(fillers.pop(0))
                for sign in (-1, 1):
                    plane = z + sign * step

                    @pl.when(is_inside & (plane >= 0) & (plane < planes))
                    def _():
                        k = plane * CORES + c
                        part = blocks.at[k, core, h]
                        arrived(k, h, sign < 0)
                        device = above if sign < 0 else below
                        if (step, c, h) == (planes - 2, CORES - 1, SPLIT - 1):
                            last_piece(k, sign < 0, device)
                        else:
                            piece(part, k, core, h, sign < 0, device).start()
                        to_mate(part, mate_recv.at[plane]).start()

    for step in range(1, planes - 1):
        relay(step)
        if step == 1:

            @pl.when(is_aide)
            def _():
                aid_out(range(SPLIT // 2))
                left_relay(range(SPLIT // 2, SPLIT))
                aid_out(range(SPLIT // 2, SPLIT))

            @pl.when(is_end)
            def _():
                for h in range(SPLIT):
                    if across:
                        across_got(h)
                    for t in range(tiles):
                        for d in across:
                            aid_up(d, t, h).start()

            second_got()

    def to_row(slot, d):
        part = sums.at[slot]
        device = ((row + jnp.where(low, d, nrow - d)) % nrow, col)
        return remote(part, part, sum_sem.at[0], sum_sem.at[1], device)

    def some_sums(number):
        part = sums.at[pl.ds(0, number)]
        return remote(part, part, sum_sem.at[0], sum_sem.at[1], mate)

    def send_sums(slot, values, weights):
        for t in range(tiles):
            sums[slot, t] = jnp.sum(values[t] * values[t], axis=0) * weights[t]
        for d in range(1, nrow):
            to_row(slot, d).start()

    def aid_own():
        for t in range(tiles):
            k = col + ncol * t
            for i in range(tiles):
                aid_acc[i] += jnp.dot(
                    square(blocks[end_row, t]), square(blocks[k, i]),
                    preferred_element_type=jnp.float32,
                )

    def aid_multiply(sources, h):
        if sources:
            for i in range(tiles):
                aid_acc[i, pl.ds(h * depth, depth)] += sum(
                    jnp.dot(
                        aid[at(*d), t, h], square(blocks[at(*d) + ncol * t, i]),
                        preferred_element_type=jnp.float32,
                    )
                    for d in sources
                    for t in range(tiles)
                )

    def inside():
        direct_products(planes - 2)

        @pl.when(is_aide)
        def _():
            aid_own()
            for h in range(SPLIT // 2):
                aid_beside_got(h)
                aid_multiply(beside, h)
            for h in range(SPLIT // 2):
                aid_across_got(h)
                aid_multiply(across, h)

        if across:
            for h in range(SPLIT):
                across_got(h)
            multiply(*((at(*d) + ncol * t, at(*d), t) for d in across for t in range(tiles)))
        send_sums(row, acc, flags)

        @pl.when(is_aide)
        def _():
            for h in range(SPLIT // 2, SPLIT):
                aid_beside_got(h)
                aid_multiply(beside, h)
                aid_across_got(h)
                aid_multiply(across, h)
            for t in range(tiles):
                stored = blocks[end_row, t, 0, pl.ds(0, 1)].astype(jnp.float32) > 0
                aid_flags[t] = jnp.where(stored, 1.0, 0.0)[0]
            send_sums(end_row, aid_acc, aid_flags)

    def outside():
        mate_own_got()

        def near(plane):
            for c in range(CORES):
                from_own(plane * CORES + c)

        planes_at(0, near)

        def nearer(up, plane):
            for h in range(SPLIT):
                for c in range(CORES):
                    k = plane * CORES + c
                    arrived(k, h, up)
                    to_mate(blocks.at[k, core, h], mate_recv.at[plane]).start()
            mate_got(plane)
            for c in range(CORES):
                from_own(plane * CORES + c)

        def farthest(up, plane):
            parts = [(h, c) for h in range(SPLIT) for c in range(CORES)]
            for h, c in parts:
                k = plane * CORES + c
                if (h, c) == parts[-1]:
                    got(last_body(k, core), recv.at[k if up else k - CORES, h])
                    to_mate(last_body(k, core), late(plane, h, c), aid_send.at[1]).start()
                    got(last_rest(k, core), last_sem.at[0])
                else:
                    arrived(k, h, up)
                    sem = z_send if h == SPLIT - 1 else mate_send
                    to_mate(blocks.at[k, core, h], late(plane, h, c), sem).start()
                multiply_piece(k, core, h)
            for h, c in parts:
                k = plane * CORES + c
                if (h, c) == parts[-1]:
                    got(last_rest(k, 1 - core), last_sem.at[1])
                    got(last_body(k, 1 - core), late(plane, h, c))
                elif h:
                    got(blocks.at[k, 1 - core, h], late(plane, h, c))
                elif c == 0:
                    both = blocks.at[pl.ds(plane * CORES, CORES), 1 - core, h]
                    got(both, late(plane, h, c))
                multiply_piece(k, 1 - core, h)

        for distance in range(1, planes):
            body = nearer if distance < top else farthest
            pl.when(z == 0)(functools.partial(body, False, distance))
            pl.when(z == top)(functools.partial(body, True, top - distance))

    pl.when(is_inside)(inside)
    pl.when(is_end)(outside)

    @pl.when(is_end)
    def _():
        some_sums(nrow).wait_recv()

    @pl.when(is_aide)
    def _():
        some_sums(nrow - 2).wait_recv()

    if planes > 4:

        @pl.when(jnp.logical_not(is_end | is_aide))
        def _():
            some_sums(nrow - 1).wait_recv()

    for s in range(tiles):
        held, slot = jnp.float32(0), jnp.int32(0)
        for t in range(tiles):
            match = cols[0, s] == col + ncol * t
            held = held + match.astype(jnp.float32)
            slot = slot + match.astype(jnp.int32) * t
        total = jnp.zeros((width,), jnp.float32)
        for t in range(tiles):
            part = sums[0, t]
            for k in range(1, nrow):
                part = part + sums[k, t]
            total = total + part * (slot == t).astype(jnp.float32)
        safe = jnp.where(total > 0, total, 1.0)
        scale = jnp.float32(0.5 * nrow * width) / safe * held
        value = acc[slot]
        out_ref[0, s] = value * value * scale[None, :] + raw[s].astype(jnp.float32) * (0.5 * held)

    def sent(part, sem):
        remote(part, part, sem, sem, mate).wait_send()

    @pl.when(is_inside)
    def _():
        sent(blocks.at[pl.ds(0, planes + 1)], z_send)
        sent(blocks.at[:, 0], mate_send)

    sent(left.at[pl.ds(0, ncol - 1)], left_send)

    @pl.when(is_end)
    def _():
        if across:
            sent(blocks.at[pl.ds(0, len(across) * tiles), 0], aid_send.at[0])
        number = len(beside) * topped + 1
        sent(aid.at[pl.ds(0, number), 0, 0, pl.ds(kept, depth - kept)], aid_send.at[1])
        sent(blocks.at[pl.ds(0, tiles * SPLIT + CORES - 1), 0, 0], z_send)
        sent(blocks.at[pl.ds(0, nrow - 1), 0], mate_send)

    @pl.when(is_inside)
    def _():
        some_sums(nrow - 1).wait_send()

    @pl.when(is_aide)
    def _():
        some_sums(nrow - 1).wait_send()
        number = len(beside) * topped + 1
        sent(aid.at[pl.ds(0, number), 0, 0, pl.ds(0, kept)], aid_send.at[1])
        if topped:
            sent(blocks.at[pl.ds(0, 3 * len(along_x)), 0], aid_send.at[0])
        else:
            sent(blocks.at[pl.ds(0, len(beside) * CORES), 0], aid_send.at[0])


def on_device(nrow, ncol, flow_tiles, tile_cols, pairs):
    _, tiles, _, width = flow_tiles.shape
    depth = width // SPLIT
    dma = pltpu.SemaphoreType.DMA
    return pl.pallas_call(
        functools.partial(kernel, nrow, ncol),
        out_shape=jax.ShapeDtypeStruct(flow_tiles.shape, jnp.float32),
        in_specs=[pl.BlockSpec(memory_space=pltpu.HBM)] * 2,
        out_specs=pl.BlockSpec(memory_space=pltpu.VMEM),
        scratch_shapes=[
            pltpu.SMEM((1, tiles), jnp.int32),
            pltpu.VMEM((tiles, width, width), jnp.bfloat16),
            pltpu.VMEM((ncol, tiles, SPLIT, depth, width), jnp.bfloat16),
            pltpu.VMEM((nrow, tiles, SPLIT, depth, width), jnp.bfloat16),
            pltpu.VMEM((ncol, tiles, SPLIT, depth, width), jnp.bfloat16),
            pltpu.VMEM((tiles, width, width), jnp.float32),
            pltpu.VMEM((tiles, width, width), jnp.float32),
            pltpu.VMEM((tiles, width), jnp.float32),
            pltpu.VMEM((tiles, width), jnp.float32),
            pltpu.VMEM((nrow, tiles, width), jnp.float32),
            dma,
            dma,
            dma((nrow - CORES, SPLIT)),
            dma((nrow // CORES + (SPLIT - 1) * CORES,)),
            dma,
            dma((2 * SPLIT + 1,)),
            dma((2,)),
            dma((2 * SPLIT,)),
            dma((2,)),
            dma((2,)),
        ],
        compiler_params=pltpu.CompilerParams(
            collective_id=0, has_side_effects=True, vmem_limit_bytes=24 * 1024 * 1024
        ),
        name="cluster_step",
    )(
        pltpu.with_memory_space_constraint(tile_cols, pltpu.HBM),
        pltpu.with_memory_space_constraint(flow_tiles, pltpu.HBM),
    )


def solution(mesh):
    placed = (P("row", "col", None, None), P("row", "col"), P(("row", "col"), None))
    return jax.shard_map(
        functools.partial(on_device, mesh.shape["row"], mesh.shape["col"]),
        mesh=mesh,
        in_specs=placed,
        out_specs=P("row", "col", None, None),
        check_vma=False,
    )
```

```python
import functools
import math

import jax
import jax.numpy as jnp
from jax import lax
from jax.experimental import pallas as pl
from jax.experimental.pallas import tpu as pltpu
from jax.sharding import PartitionSpec as P

MESH = pl.DeviceIdType.MESH
CORES = 2
SPLIT = 2


def remote(src, dst, send_sem, recv_sem, device):
    return pltpu.make_async_remote_copy(
        src_ref=src,
        dst_ref=dst,
        send_sem=send_sem,
        recv_sem=recv_sem,
        device_id=device,
        device_id_type=MESH,
    )


def kernel(
    nrow, ncol, cols_hbm, flow_hbm, out_ref,
    cols, raw, left, blocks, aid, acc, aid_acc, flags, aid_flags, sums,
    z_send, mate_send, recv, mate_recv, left_send, left_recv,
    aid_send, aid_recv, sum_sem, last_sem,
):
    tiles, width = raw.shape[0], raw.shape[2]
    depth = left.shape[3]
    planes = nrow // CORES
    row, col = lax.axis_index("row"), lax.axis_index("col")
    z, core = row // CORES, row % CORES
    mate_row = row + 1 - 2 * core
    mate = (mate_row, col)
    above, below = (row + CORES, col), (row - CORES, col)
    has_above, has_below = z < planes - 1, z > 0
    ny = math.isqrt(ncol)
    ny = ny if ny * ny == ncol else 1
    nx = ncol // ny
    y, x = col // nx, col % nx
    half = tiles // 2
    top = planes - 1
    is_end = (z == 0) | (z == top)
    is_inside = jnp.logical_not(is_end)
    is_aide = (z == 1) | (z == top - 1)
    end_row = jnp.where(z <= 1, 0, top) * CORES + core
    inner_row = jnp.where(z == 0, 1, top - 1) * CORES + core

    def at(dy, dx):
        return ((y + dy) % ny) * nx + (x + dx) % nx

    along_x = [(0, dx) for dx in range(1, nx)]
    along_y = [(dy, 0) for dy in range(1, ny)]
    beside = along_x + along_y
    across = [(dy, dx) for dy, _ in along_y for _, dx in along_x]
    firsts = [(d, t) for t in range(half) for d in along_x]
    firsts += [(d, t) for t in range(half, tiles) for d in along_y]
    seconds = [(d, t) for t in range(half, tiles) for d in along_x]
    seconds += [(d, t) for t in range(half) for d in along_y]
    topped = nx == ny and tiles == CORES
    kept = depth // 4
    spare = kept

    load_cols = pltpu.make_async_copy(cols_hbm, cols, left_send)
    load_flow = pltpu.make_async_copy(flow_hbm.at[0], raw, mate_send)
    load_cols.start()
    load_flow.start()

    barrier = pltpu.get_barrier_semaphore()

    def greet(device):
        pl.semaphore_signal(barrier, inc=1, device_id=device, device_id_type=MESH)

    greet(mate)
    for d in beside:
        greet((row, at(*d)))
        greet((mate_row, at(*d)))

    @pl.when(has_above)
    def _():
        for c in range(CORES):
            greet(((z + 1) * CORES + c, col))

    @pl.when(has_below)
    def _():
        for c in range(CORES):
            greet(((z - 1) * CORES + c, col))

    load_cols.wait()
    load_flow.wait()
    for t in range(tiles):
        target = col + ncol * t
        tile = jnp.zeros((width, width), jnp.float32)
        weight = jnp.float32(0)
        for s in range(tiles):
            w = (cols[0, s] == target).astype(jnp.float32)
            weight = weight + w
            tile = tile + raw[s].astype(jnp.float32) * w
        flags[t] = jnp.full((width,), weight, jnp.float32)
        tile = tile.astype(jnp.bfloat16).reshape(SPLIT, depth, width)
        left[col, t] = tile
        blocks[row, t] = tile

    ends = jnp.where(has_above, 1, 0) + jnp.where(has_below, 1, 0)
    pl.semaphore_wait(barrier, 1 + CORES * (len(beside) + ends))

    def piece(src, k, t, h, up, device):
        index = k if up else k - CORES
        send_sem = z_send
        return remote(src, blocks.at[k, t, h], send_sem, recv.at[index, h], device)

    def arrived(k, h, up):
        piece(blocks.at[k, core, h], k, core, h, up, mate).wait_recv()

    def last_piece(k, up, device):
        send_sem = z_send
        body, rest = last_body(k, core), last_rest(k, core)
        index = k if up else k - CORES
        remote(body, body, send_sem, recv.at[index, SPLIT - 1], device).start()
        remote(rest, rest, send_sem, last_sem.at[0], device).start()
        other = (device[0] + 1 - 2 * core, col)
        remote(rest, rest, aid_send.at[1], last_sem.at[1], other).start()

    def last_body(k, t):
        return blocks.at[k, t, SPLIT - 1, pl.ds(0, depth - spare)]

    def last_rest(k, t):
        return blocks.at[k, t, SPLIT - 1, pl.ds(depth - spare, spare)]

    def to_mate(part, arrival, sem=mate_send):
        return remote(part, part, sem, arrival, mate)

    def mate_got(plane):
        part = blocks.at[pl.ds(plane * CORES, CORES), 1 - core]
        to_mate(part, mate_recv.at[plane]).wait_recv()

    def late(plane, h, c):
        return mate_recv.at[plane if h == 0 else top + (h - 1) * CORES + c + 1]

    def got(part, sem):
        remote(part, part, sem, sem, mate).wait_recv()

    def left_out(source, move, t, h):
        part = left.at[at(*source), t, h]
        if source != (0, 0):
            kind = SPLIT + h
        else:
            kind = h if (move, t) in firsts else 2 * SPLIT
        return remote(part, part, left_send, left_recv.at[kind], (row, at(*move)))

    def first_got(h):
        got(left.at[pl.ds(0, len(firsts)), 0, 0], left_recv.at[h])

    def second_got():
        got(left.at[pl.ds(0, len(seconds)), 0], left_recv.at[2 * SPLIT])

    def across_got(h):
        got(left.at[pl.ds(0, len(across)), :, 0], left_recv.at[SPLIT + h])

    def left_relay(halves):
        for h in halves:
            for d, t in firsts:
                for move in along_y if t < half else along_x:
                    left_out(d, move, t, h).start()

    def left_rest():
        for d, t in seconds:
            for h in range(SPLIT):
                left_out((0, 0), d, t, h).start()

    def aid_up(d, t, h):
        part = left.at[at(*d), t, h]
        arrival = aid_recv.at[h]
        return remote(part, aid.at[at(*d), t, h], aid_send.at[0], arrival, (inner_row, col))

    def top_up():
        for d, t in firsts:
            part = left.at[at(*d), t, SPLIT - 1, pl.ds(kept, depth - kept)]
            target = aid.at[at(*d), t, SPLIT - 1, pl.ds(kept, depth - kept)]
            arrival = aid_recv.at[SPLIT - 1]
            remote(part, target, aid_send.at[1], arrival, (inner_row, col)).start()

    def aid_out(halves):
        def send(h, c, sources, number=depth, sem=aid_send.at[0]):
            part = blocks.at[end_row - core + c, core, h, pl.ds(0, number)]
            target = aid.at[col, core, h, pl.ds(0, number)]
            for d in sources:
                device = (z * CORES + c, at(*d))
                remote(part, target, sem, aid_recv.at[h], device).start()

        def send_late(h, c, by_top, others):
            send(h, c, others)
            send(h, c, by_top, kept, aid_send.at[1])

        for h in halves:
            for c in range(CORES):
                if topped and h == SPLIT - 1:
                    pl.when(core < half)(functools.partial(send_late, h, c, along_x, along_y))
                    pl.when(core >= half)(functools.partial(send_late, h, c, along_y, along_x))
                else:
                    send(h, c, beside)

    def aid_got(h):
        got(aid.at[pl.ds(0, ncol - 1), :, 0], aid_recv.at[h])

    own_to_mate = remote(left.at[col], blocks.at[row], mate_send, mate_recv.at[z], mate)

    def own_up(t, h):
        @pl.when(has_above)
        def _():
            device = ((z + 1) * CORES + t, col)
            piece(left.at[col, t, h], row, t, h, True, device).start()

    def own_down(t, h):
        @pl.when(has_below)
        def _():
            device = ((z - 1) * CORES + t, col)
            piece(left.at[col, t, h], row, t, h, False, device).start()

    low = z < top - z
    for h in range(SPLIT):
        for t in range(tiles):

            @pl.when(low)
            def _():
                own_down(t, h)

            own_up(t, h)

            @pl.when(jnp.logical_not(low))
            def _():
                own_down(t, h)

        if h == 0:
            for d, t in firsts:
                for g in range(SPLIT):
                    left_out((0, 0), d, t, g).start()

            @pl.when(is_inside)
            def _():
                left_rest()

    own_to_mate.start()

    acc[...] = jnp.zeros_like(acc)
    aid_acc[...] = jnp.zeros_like(aid_acc)

    def square(part):
        return part.reshape(-1, width)

    def multiply(*terms):
        for t in range(tiles):
            acc[t] += sum(
                jnp.dot(
                    square(left[c, i]), square(blocks[k, t]), preferred_element_type=jnp.float32
                )
                for k, c, i in terms
            )

    def multiply_piece(k, t, h):
        a = left[k % ncol, k // ncol, :, :, pl.ds(h * depth, depth)]
        acc[t] += jnp.dot(
            a.reshape(width, depth), blocks[k, t, h], preferred_element_type=jnp.float32
        )

    def from_own(k):
        multiply((k, k % ncol, k // ncol))

    def is_direct(k):
        c = k % ncol
        return (c // nx == y) | (c % nx == x)

    def planes_at(distance, body):
        for sign in (-1, 1) if distance else (1,):
            plane = z + sign * distance
            pl.when((plane >= 0) & (plane < planes))(functools.partial(body, plane))

    def direct_products(distance):
        def run(plane):
            if distance:
                mate_got(plane)
            for c in range(CORES):
                k = plane * CORES + c

                @pl.when(is_direct(k))
                def _():
                    from_own(k)

        planes_at(distance, run)

    def mate_own_got():
        got(blocks.at[mate_row], mate_recv.at[z])

    fillers = []

    def first_filler():
        mate_own_got()
        direct_products(0)

    if planes > 3:
        fillers.append(first_filler)
        for distance in range(1, planes - 2):
            fillers.append(functools.partial(direct_products, distance))

    def relay(step):
        for h in range(SPLIT):
            if step == 1 and h == SPLIT - 1:
                for g in range(SPLIT):
                    first_got(g)
                    if g < SPLIT // 2:
                        left_relay([g])
                    else:
                        pl.when(jnp.logical_not(is_aide))(functools.partial(left_relay, [g]))
                if topped:
                    pl.when(is_end)(top_up)
                pl.when(is_end)(left_rest)

            for c in range(CORES):
                if step == planes - 2:
                    number = SPLIT * CORES - (h * CORES + c)
                    for _ in range(-(-len(fillers) // number)):
                        pl.when(is_inside)(fillers.pop(0))
                for sign in (-1, 1):
                    plane = z + sign * step

                    @pl.when(is_inside & (plane >= 0) & (plane < planes))
                    def _():
                        k = plane * CORES + c
                        part = blocks.at[k, core, h]
                        arrived(k, h, sign < 0)
                        device = above if sign < 0 else below
                        if (step, c, h) == (planes - 2, CORES - 1, SPLIT - 1):
                            last_piece(k, sign < 0, device)
                        else:
                            piece(part, k, core, h, sign < 0, device).start()
                        to_mate(part, mate_recv.at[plane]).start()

    for step in range(1, planes - 1):
        relay(step)
        if step == 1:

            @pl.when(is_aide)
            def _():
                aid_out(range(SPLIT // 2))
                left_relay(range(SPLIT // 2, SPLIT))
                aid_out(range(SPLIT // 2, SPLIT))

            @pl.when(is_end)
            def _():
                for h in range(SPLIT):
                    if across:
                        across_got(h)
                    for t in range(tiles):
                        for d in across:
                            aid_up(d, t, h).start()

            second_got()

    def to_row(slot, d):
        part = sums.at[slot]
        device = ((row + jnp.where(low, d, nrow - d)) % nrow, col)
        return remote(part, part, sum_sem.at[0], sum_sem.at[1], device)

    def some_sums(number):
        part = sums.at[pl.ds(0, number)]
        return remote(part, part, sum_sem.at[0], sum_sem.at[1], mate)

    def send_sums(slot, values, weights):
        for t in range(tiles):
            sums[slot, t] = jnp.sum(values[t] * values[t], axis=0) * weights[t]
        for d in range(1, nrow):
            to_row(slot, d).start()

    def aid_own():
        for t in range(tiles):
            k = col + ncol * t
            for i in range(tiles):
                aid_acc[i] += jnp.dot(
                    square(blocks[end_row, t]), square(blocks[k, i]),
                    preferred_element_type=jnp.float32,
                )

    def aid_multiply(sources, h):
        if sources:
            for i in range(tiles):
                aid_acc[i, pl.ds(h * depth, depth)] += sum(
                    jnp.dot(
                        aid[at(*d), t, h], square(blocks[at(*d) + ncol * t, i]),
                        preferred_element_type=jnp.float32,
                    )
                    for d in sources
                    for t in range(tiles)
                )

    def inside():
        direct_products(planes - 2)

        @pl.when(is_aide)
        def _():
            aid_own()
            for h in range(SPLIT // 2):
                aid_got(h)
                aid_multiply(beside + across, h)

        if across:
            for h in range(SPLIT):
                across_got(h)
            multiply(*((at(*d) + ncol * t, at(*d), t) for d in across for t in range(tiles)))
        send_sums(row, acc, flags)

        @pl.when(is_aide)
        def _():
            for h in range(SPLIT // 2, SPLIT):
                aid_got(h)
                aid_multiply(beside + across, h)
            for t in range(tiles):
                stored = blocks[end_row, t, 0, pl.ds(0, 1)].astype(jnp.float32) > 0
                aid_flags[t] = jnp.where(stored, 1.0, 0.0)[0]
            send_sums(end_row, aid_acc, aid_flags)

    def outside():
        mate_own_got()

        def near(plane):
            for c in range(CORES):
                from_own(plane * CORES + c)

        planes_at(0, near)

        def nearer(up, plane):
            for h in range(SPLIT):
                for c in range(CORES):
                    k = plane * CORES + c
                    arrived(k, h, up)
                    to_mate(blocks.at[k, core, h], mate_recv.at[plane]).start()
            mate_got(plane)
            for c in range(CORES):
                from_own(plane * CORES + c)

        def farthest(up, plane):
            parts = [(h, c) for h in range(SPLIT) for c in range(CORES)]
            for h, c in parts:
                k = plane * CORES + c
                if (h, c) == parts[-1]:
                    got(last_body(k, core), recv.at[k if up else k - CORES, h])
                    to_mate(last_body(k, core), late(plane, h, c), aid_send.at[1]).start()
                    got(last_rest(k, core), last_sem.at[0])
                else:
                    arrived(k, h, up)
                    sem = z_send if h == SPLIT - 1 else mate_send
                    to_mate(blocks.at[k, core, h], late(plane, h, c), sem).start()
                multiply_piece(k, core, h)
            for h, c in parts:
                k = plane * CORES + c
                if (h, c) == parts[-1]:
                    got(last_rest(k, 1 - core), last_sem.at[1])
                    got(last_body(k, 1 - core), late(plane, h, c))
                elif h:
                    got(blocks.at[k, 1 - core, h], late(plane, h, c))
                elif c == 0:
                    both = blocks.at[pl.ds(plane * CORES, CORES), 1 - core, h]
                    got(both, late(plane, h, c))
                multiply_piece(k, 1 - core, h)

        for distance in range(1, planes):
            body = nearer if distance < top else farthest
            pl.when(z == 0)(functools.partial(body, False, distance))
            pl.when(z == top)(functools.partial(body, True, top - distance))

    pl.when(is_inside)(inside)
    pl.when(is_end)(outside)

    @pl.when(is_end)
    def _():
        some_sums(nrow).wait_recv()

    @pl.when(is_aide)
    def _():
        some_sums(nrow - 2).wait_recv()

    if planes > 4:

        @pl.when(jnp.logical_not(is_end | is_aide))
        def _():
            some_sums(nrow - 1).wait_recv()

    for s in range(tiles):
        held, slot = jnp.float32(0), jnp.int32(0)
        for t in range(tiles):
            match = cols[0, s] == col + ncol * t
            held = held + match.astype(jnp.float32)
            slot = slot + match.astype(jnp.int32) * t
        total = jnp.zeros((width,), jnp.float32)
        for t in range(tiles):
            part = sums[0, t]
            for k in range(1, nrow):
                part = part + sums[k, t]
            total = total + part * (slot == t).astype(jnp.float32)
        safe = jnp.where(total > 0, total, 1.0)
        scale = jnp.float32(0.5 * nrow * width) / safe * held
        value = acc[slot]
        out_ref[0, s] = value * value * scale[None, :] + raw[s].astype(jnp.float32) * (0.5 * held)

    def sent(part, sem):
        remote(part, part, sem, sem, mate).wait_send()

    @pl.when(is_inside)
    def _():
        sent(blocks.at[pl.ds(0, planes + 1)], z_send)
        sent(blocks.at[:, 0], mate_send)

    sent(left.at[pl.ds(0, ncol - 1)], left_send)

    @pl.when(is_end)
    def _():
        if across:
            sent(blocks.at[pl.ds(0, len(across) * tiles), 0], aid_send.at[0])
        number = len(beside) * topped + 1
        sent(aid.at[pl.ds(0, number), 0, 0, pl.ds(kept, depth - kept)], aid_send.at[1])
        sent(blocks.at[pl.ds(0, tiles * SPLIT + CORES - 1), 0, 0], z_send)
        sent(blocks.at[pl.ds(0, nrow - 1), 0], mate_send)

    @pl.when(is_inside)
    def _():
        some_sums(nrow - 1).wait_send()

    @pl.when(is_aide)
    def _():
        some_sums(nrow - 1).wait_send()
        number = len(beside) * topped + 1
        sent(aid.at[pl.ds(0, number), 0, 0, pl.ds(0, kept)], aid_send.at[1])
        if topped:
            sent(blocks.at[pl.ds(0, 3 * len(along_x)), 0], aid_send.at[0])
        else:
            sent(blocks.at[pl.ds(0, len(beside) * CORES), 0], aid_send.at[0])


def on_device(nrow, ncol, flow_tiles, tile_cols, pairs):
    _, tiles, _, width = flow_tiles.shape
    depth = width // SPLIT
    dma = pltpu.SemaphoreType.DMA
    return pl.pallas_call(
        functools.partial(kernel, nrow, ncol),
        out_shape=jax.ShapeDtypeStruct(flow_tiles.shape, jnp.float32),
        in_specs=[pl.BlockSpec(memory_space=pltpu.HBM)] * 2,
        out_specs=pl.BlockSpec(memory_space=pltpu.VMEM),
        scratch_shapes=[
            pltpu.SMEM((1, tiles), jnp.int32),
            pltpu.VMEM((tiles, width, width), jnp.bfloat16),
            pltpu.VMEM((ncol, tiles, SPLIT, depth, width), jnp.bfloat16),
            pltpu.VMEM((nrow, tiles, SPLIT, depth, width), jnp.bfloat16),
            pltpu.VMEM((ncol, tiles, SPLIT, depth, width), jnp.bfloat16),
            pltpu.VMEM((tiles, width, width), jnp.float32),
            pltpu.VMEM((tiles, width, width), jnp.float32),
            pltpu.VMEM((tiles, width), jnp.float32),
            pltpu.VMEM((tiles, width), jnp.float32),
            pltpu.VMEM((nrow, tiles, width), jnp.float32),
            dma,
            dma,
            dma((nrow - CORES, SPLIT)),
            dma((nrow // CORES + (SPLIT - 1) * CORES,)),
            dma,
            dma((2 * SPLIT + 1,)),
            dma((2,)),
            dma((SPLIT,)),
            dma((2,)),
            dma((2,)),
        ],
        compiler_params=pltpu.CompilerParams(
            collective_id=0, has_side_effects=True, vmem_limit_bytes=24 * 1024 * 1024
        ),
        name="cluster_step",
    )(
        pltpu.with_memory_space_constraint(tile_cols, pltpu.HBM),
        pltpu.with_memory_space_constraint(flow_tiles, pltpu.HBM),
    )


def solution(mesh):
    placed = (P("row", "col", None, None), P("row", "col"), P(("row", "col"), None))
    return jax.shard_map(
        functools.partial(on_device, mesh.shape["row"], mesh.shape["col"]),
        mesh=mesh,
        in_specs=placed,
        out_specs=P("row", "col", None, None),
        check_vma=False,
    )
```

```python
import functools
import math

import jax
import jax.numpy as jnp
from jax import lax
from jax.experimental import pallas as pl
from jax.experimental.pallas import tpu as pltpu
from jax.sharding import PartitionSpec as P

MESH = pl.DeviceIdType.MESH
CORES = 2
SPLIT = 2


def remote(src, dst, send_sem, recv_sem, device):
    return pltpu.make_async_remote_copy(
        src_ref=src,
        dst_ref=dst,
        send_sem=send_sem,
        recv_sem=recv_sem,
        device_id=device,
        device_id_type=MESH,
    )


def kernel(
    nrow, ncol, cols_hbm, flow_hbm, out_ref,
    cols, raw, left, blocks, aid, acc, aid_acc, flags, aid_flags, sums,
    z_send, mate_send, recv, mate_recv, left_send, left_recv,
    aid_send, aid_recv, sum_sem, last_sem,
):
    tiles, width = raw.shape[0], raw.shape[2]
    depth = left.shape[3]
    planes = nrow // CORES
    row, col = lax.axis_index("row"), lax.axis_index("col")
    z, core = row // CORES, row % CORES
    mate_row = row + 1 - 2 * core
    mate = (mate_row, col)
    above, below = (row + CORES, col), (row - CORES, col)
    has_above, has_below = z < planes - 1, z > 0
    ny = math.isqrt(ncol)
    ny = ny if ny * ny == ncol else 1
    nx = ncol // ny
    y, x = col // nx, col % nx
    half = tiles // 2
    top = planes - 1
    is_end = (z == 0) | (z == top)
    is_inside = jnp.logical_not(is_end)
    is_aide = (z == 1) | (z == top - 1)
    end_row = jnp.where(z <= 1, 0, top) * CORES + core
    inner_row = jnp.where(z == 0, 1, top - 1) * CORES + core

    def at(dy, dx):
        return ((y + dy) % ny) * nx + (x + dx) % nx

    along_x = [(0, dx) for dx in range(1, nx)]
    along_y = [(dy, 0) for dy in range(1, ny)]
    beside = along_x + along_y
    across = [(dy, dx) for dy, _ in along_y for _, dx in along_x]
    firsts = [(d, t) for t in range(half) for d in along_x]
    firsts += [(d, t) for t in range(half, tiles) for d in along_y]
    seconds = [(d, t) for t in range(half, tiles) for d in along_x]
    seconds += [(d, t) for t in range(half) for d in along_y]
    topped = nx == ny and tiles == CORES
    kept = depth // 4
    spare = kept

    load_cols = pltpu.make_async_copy(cols_hbm, cols, left_send)
    load_flow = pltpu.make_async_copy(flow_hbm.at[0], raw, mate_send)
    load_cols.start()
    load_flow.start()

    barrier = pltpu.get_barrier_semaphore()

    def greet(device):
        pl.semaphore_signal(barrier, inc=1, device_id=device, device_id_type=MESH)

    greet(mate)
    for d in beside:
        greet((row, at(*d)))
        greet((mate_row, at(*d)))

    @pl.when(has_above)
    def _():
        for c in range(CORES):
            greet(((z + 1) * CORES + c, col))

    @pl.when(has_below)
    def _():
        for c in range(CORES):
            greet(((z - 1) * CORES + c, col))

    load_cols.wait()
    load_flow.wait()
    for t in range(tiles):
        target = col + ncol * t
        tile = jnp.zeros((width, width), jnp.float32)
        weight = jnp.float32(0)
        for s in range(tiles):
            w = (cols[0, s] == target).astype(jnp.float32)
            weight = weight + w
            tile = tile + raw[s].astype(jnp.float32) * w
        flags[t] = jnp.full((width,), weight, jnp.float32)
        tile = tile.astype(jnp.bfloat16).reshape(SPLIT, depth, width)
        left[col, t] = tile
        blocks[row, t] = tile

    ends = jnp.where(has_above, 1, 0) + jnp.where(has_below, 1, 0)
    pl.semaphore_wait(barrier, 1 + CORES * (len(beside) + ends))

    def piece(src, k, t, h, up, device):
        index = k if up else k - CORES
        send_sem = z_send
        return remote(src, blocks.at[k, t, h], send_sem, recv.at[index, h], device)

    def arrived(k, h, up):
        piece(blocks.at[k, core, h], k, core, h, up, mate).wait_recv()

    def last_piece(k, up, device):
        send_sem = z_send
        body, rest = last_body(k, core), last_rest(k, core)
        index = k if up else k - CORES
        remote(body, body, send_sem, recv.at[index, SPLIT - 1], device).start()
        remote(rest, rest, send_sem, last_sem.at[0], device).start()
        other = (device[0] + 1 - 2 * core, col)
        remote(rest, rest, aid_send.at[1], last_sem.at[1], other).start()

    def last_body(k, t):
        return blocks.at[k, t, SPLIT - 1, pl.ds(0, depth - spare)]

    def last_rest(k, t):
        return blocks.at[k, t, SPLIT - 1, pl.ds(depth - spare, spare)]

    def to_mate(part, arrival, sem=mate_send):
        return remote(part, part, sem, arrival, mate)

    def mate_got(plane):
        part = blocks.at[pl.ds(plane * CORES, CORES), 1 - core]
        to_mate(part, mate_recv.at[plane]).wait_recv()

    def late(plane, h, c):
        return mate_recv.at[plane if h == 0 else top + (h - 1) * CORES + c + 1]

    def got(part, sem):
        remote(part, part, sem, sem, mate).wait_recv()

    def left_out(source, move, t, h):
        part = left.at[at(*source), t, h]
        if source != (0, 0):
            kind = SPLIT + h
        else:
            kind = h if (move, t) in firsts else 2 * SPLIT
        return remote(part, part, left_send, left_recv.at[kind], (row, at(*move)))

    def first_got(h):
        got(left.at[pl.ds(0, len(firsts)), 0, 0], left_recv.at[h])

    def second_got():
        got(left.at[pl.ds(0, len(seconds)), 0], left_recv.at[2 * SPLIT])

    def across_got(h):
        got(left.at[pl.ds(0, len(across)), :, 0], left_recv.at[SPLIT + h])

    def left_relay(halves):
        for h in halves:
            for d, t in firsts:
                for move in along_y if t < half else along_x:
                    left_out(d, move, t, h).start()

    def left_rest():
        for d, t in seconds:
            for h in range(SPLIT):
                left_out((0, 0), d, t, h).start()

    def aid_up(d, t, h):
        part = left.at[at(*d), t, h]
        arrival = aid_recv.at[SPLIT + h]
        return remote(part, aid.at[at(*d), t, h], aid_send.at[0], arrival, (inner_row, col))

    def top_up():
        for d, t in firsts:
            part = left.at[at(*d), t, SPLIT - 1, pl.ds(kept, depth - kept)]
            target = aid.at[at(*d), t, SPLIT - 1, pl.ds(kept, depth - kept)]
            arrival = aid_recv.at[SPLIT - 1]
            remote(part, target, aid_send.at[1], arrival, (inner_row, col)).start()

    def aid_out(halves):
        def send(h, c, sources, number=depth, sem=aid_send.at[0]):
            part = blocks.at[end_row - core + c, core, h, pl.ds(0, number)]
            target = aid.at[col, core, h, pl.ds(0, number)]
            for d in sources:
                device = (z * CORES + c, at(*d))
                remote(part, target, sem, aid_recv.at[h], device).start()

        def send_late(h, c, by_top, others):
            send(h, c, others)
            send(h, c, by_top, kept, aid_send.at[1])

        for h in halves:
            for c in range(CORES):
                if topped and h == SPLIT - 1:
                    pl.when(core < half)(functools.partial(send_late, h, c, along_x, along_y))
                    pl.when(core >= half)(functools.partial(send_late, h, c, along_y, along_x))
                else:
                    send(h, c, beside)

    def aid_beside_got(h):
        got(aid.at[pl.ds(0, len(beside)), :, 0], aid_recv.at[h])

    def aid_across_got(h):
        if across:
            got(aid.at[pl.ds(0, len(across)), :, 0], aid_recv.at[SPLIT + h])

    own_to_mate = remote(left.at[col], blocks.at[row], mate_send, mate_recv.at[z], mate)

    def own_up(t, h):
        @pl.when(has_above)
        def _():
            device = ((z + 1) * CORES + t, col)
            piece(left.at[col, t, h], row, t, h, True, device).start()

    def own_down(t, h):
        @pl.when(has_below)
        def _():
            device = ((z - 1) * CORES + t, col)
            piece(left.at[col, t, h], row, t, h, False, device).start()

    low = z < top - z
    for h in range(SPLIT):
        for t in range(tiles):

            @pl.when(low)
            def _():
                own_down(t, h)

            own_up(t, h)

            @pl.when(jnp.logical_not(low))
            def _():
                own_down(t, h)

        if h == 0:
            for d, t in firsts:
                for g in range(SPLIT):
                    left_out((0, 0), d, t, g).start()

            @pl.when(is_inside)
            def _():
                left_rest()

    own_to_mate.start()

    acc[...] = jnp.zeros_like(acc)
    aid_acc[...] = jnp.zeros_like(aid_acc)

    def square(part):
        return part.reshape(-1, width)

    def multiply(*terms):
        for t in range(tiles):
            acc[t] += sum(
                jnp.dot(
                    square(left[c, i]), square(blocks[k, t]), preferred_element_type=jnp.float32
                )
                for k, c, i in terms
            )

    def multiply_piece(k, t, h):
        a = left[k % ncol, k // ncol, :, :, pl.ds(h * depth, depth)]
        acc[t] += jnp.dot(
            a.reshape(width, depth), blocks[k, t, h], preferred_element_type=jnp.float32
        )

    def from_own(k):
        multiply((k, k % ncol, k // ncol))

    def is_direct(k):
        c = k % ncol
        return (c // nx == y) | (c % nx == x)

    def planes_at(distance, body):
        for sign in (-1, 1) if distance else (1,):
            plane = z + sign * distance
            pl.when((plane >= 0) & (plane < planes))(functools.partial(body, plane))

    def direct_products(distance):
        def run(plane):
            if distance:
                mate_got(plane)
            for c in range(CORES):
                k = plane * CORES + c

                @pl.when(is_direct(k))
                def _():
                    from_own(k)

        planes_at(distance, run)

    def mate_own_got():
        got(blocks.at[mate_row], mate_recv.at[z])

    fillers = []

    def first_filler():
        mate_own_got()
        direct_products(0)

    if planes > 3:
        fillers.append(first_filler)
        for distance in range(1, planes - 2):
            fillers.append(functools.partial(direct_products, distance))

    def relay(step):
        for h in range(SPLIT):
            if step == 1 and h == SPLIT - 1:
                for g in range(SPLIT):
                    first_got(g)
                    if g < SPLIT // 2:
                        left_relay([g])
                    else:
                        pl.when(jnp.logical_not(is_aide))(functools.partial(left_relay, [g]))
                if topped:
                    pl.when(is_end)(top_up)
                pl.when(is_end)(left_rest)

            for c in range(CORES):
                if step == planes - 2:
                    number = SPLIT * CORES - (h * CORES + c)
                    for _ in range(-(-len(fillers) // number)):
                        pl.when(is_inside)(fillers.pop(0))
                for sign in (1, -1):
                    plane = z + sign * step

                    @pl.when(is_inside & (plane >= 0) & (plane < planes))
                    def _():
                        k = plane * CORES + c
                        part = blocks.at[k, core, h]
                        arrived(k, h, sign < 0)
                        device = above if sign < 0 else below
                        if (step, c, h) == (planes - 2, CORES - 1, SPLIT - 1):
                            last_piece(k, sign < 0, device)
                        else:
                            piece(part, k, core, h, sign < 0, device).start()
                        to_mate(part, mate_recv.at[plane]).start()

    for step in range(1, planes - 1):
        relay(step)
        if step == 1:

            @pl.when(is_aide)
            def _():
                aid_out(range(SPLIT // 2))
                left_relay(range(SPLIT // 2, SPLIT))
                aid_out(range(SPLIT // 2, SPLIT))

            @pl.when(is_end)
            def _():
                for h in range(SPLIT):
                    if across:
                        across_got(h)
                    for t in range(tiles):
                        for d in across:
                            aid_up(d, t, h).start()

            second_got()

    def to_row(slot, d):
        part = sums.at[slot]
        device = ((row + jnp.where(low, d, nrow - d)) % nrow, col)
        return remote(part, part, sum_sem.at[0], sum_sem.at[1], device)

    def some_sums(number):
        part = sums.at[pl.ds(0, number)]
        return remote(part, part, sum_sem.at[0], sum_sem.at[1], mate)

    def send_sums(slot, values, weights):
        for t in range(tiles):
            sums[slot, t] = jnp.sum(values[t] * values[t], axis=0) * weights[t]
        for d in range(1, nrow):
            to_row(slot, d).start()

    def aid_own():
        for t in range(tiles):
            k = col + ncol * t
            for i in range(tiles):
                aid_acc[i] += jnp.dot(
                    square(blocks[end_row, t]), square(blocks[k, i]),
                    preferred_element_type=jnp.float32,
                )

    def aid_multiply(sources, h):
        if sources:
            for i in range(tiles):
                aid_acc[i, pl.ds(h * depth, depth)] += sum(
                    jnp.dot(
                        aid[at(*d), t, h], square(blocks[at(*d) + ncol * t, i]),
                        preferred_element_type=jnp.float32,
                    )
                    for d in sources
                    for t in range(tiles)
                )

    def inside():
        direct_products(planes - 2)

        @pl.when(is_aide)
        def _():
            aid_own()
            for h in range(SPLIT // 2):
                aid_beside_got(h)
                aid_multiply(beside, h)
            for h in range(SPLIT // 2):
                aid_across_got(h)
                aid_multiply(across, h)

        if across:
            for h in range(SPLIT):
                across_got(h)
            multiply(*((at(*d) + ncol * t, at(*d), t) for d in across for t in range(tiles)))
        send_sums(row, acc, flags)

        @pl.when(is_aide)
        def _():
            for h in range(SPLIT // 2, SPLIT):
                aid_beside_got(h)
                aid_multiply(beside, h)
                aid_across_got(h)
                aid_multiply(across, h)
            for t in range(tiles):
                stored = blocks[end_row, t, 0, pl.ds(0, 1)].astype(jnp.float32) > 0
                aid_flags[t] = jnp.where(stored, 1.0, 0.0)[0]
            send_sums(end_row, aid_acc, aid_flags)

    def outside():
        mate_own_got()

        def near(plane):
            for c in range(CORES):
                from_own(plane * CORES + c)

        planes_at(0, near)

        def nearer(up, plane):
            for h in range(SPLIT):
                for c in range(CORES):
                    k = plane * CORES + c
                    arrived(k, h, up)
                    to_mate(blocks.at[k, core, h], mate_recv.at[plane]).start()
            mate_got(plane)
            for c in range(CORES):
                from_own(plane * CORES + c)

        def farthest(up, plane):
            parts = [(h, c) for h in range(SPLIT) for c in range(CORES)]
            for h, c in parts:
                k = plane * CORES + c
                if (h, c) == parts[-1]:
                    got(last_body(k, core), recv.at[k if up else k - CORES, h])
                    to_mate(last_body(k, core), late(plane, h, c), aid_send.at[1]).start()
                    got(last_rest(k, core), last_sem.at[0])
                else:
                    arrived(k, h, up)
                    sem = z_send if h == SPLIT - 1 else mate_send
                    to_mate(blocks.at[k, core, h], late(plane, h, c), sem).start()
                multiply_piece(k, core, h)
            for h, c in parts:
                k = plane * CORES + c
                if (h, c) == parts[-1]:
                    got(last_rest(k, 1 - core), last_sem.at[1])
                    got(last_body(k, 1 - core), late(plane, h, c))
                elif h:
                    got(blocks.at[k, 1 - core, h], late(plane, h, c))
                elif c == 0:
                    both = blocks.at[pl.ds(plane * CORES, CORES), 1 - core, h]
                    got(both, late(plane, h, c))
                multiply_piece(k, 1 - core, h)

        for distance in range(1, planes):
            body = nearer if distance < top else farthest
            pl.when(z == 0)(functools.partial(body, False, distance))
            pl.when(z == top)(functools.partial(body, True, top - distance))

    pl.when(is_inside)(inside)
    pl.when(is_end)(outside)

    @pl.when(is_end)
    def _():
        some_sums(nrow).wait_recv()

    @pl.when(is_aide)
    def _():
        some_sums(nrow - 2).wait_recv()

    if planes > 4:

        @pl.when(jnp.logical_not(is_end | is_aide))
        def _():
            some_sums(nrow - 1).wait_recv()

    for s in range(tiles):
        held, slot = jnp.float32(0), jnp.int32(0)
        for t in range(tiles):
            match = cols[0, s] == col + ncol * t
            held = held + match.astype(jnp.float32)
            slot = slot + match.astype(jnp.int32) * t
        total = jnp.zeros((width,), jnp.float32)
        for t in range(tiles):
            part = sums[0, t]
            for k in range(1, nrow):
                part = part + sums[k, t]
            total = total + part * (slot == t).astype(jnp.float32)
        safe = jnp.where(total > 0, total, 1.0)
        scale = jnp.float32(0.5 * nrow * width) / safe * held
        value = acc[slot]
        out_ref[0, s] = value * value * scale[None, :] + raw[s].astype(jnp.float32) * (0.5 * held)

    def sent(part, sem):
        remote(part, part, sem, sem, mate).wait_send()

    @pl.when(is_inside)
    def _():
        sent(blocks.at[pl.ds(0, planes + 1)], z_send)
        sent(blocks.at[:, 0], mate_send)

    sent(left.at[pl.ds(0, ncol - 1)], left_send)

    @pl.when(is_end)
    def _():
        if across:
            sent(blocks.at[pl.ds(0, len(across) * tiles), 0], aid_send.at[0])
        number = len(beside) * topped + 1
        sent(aid.at[pl.ds(0, number), 0, 0, pl.ds(kept, depth - kept)], aid_send.at[1])
        sent(blocks.at[pl.ds(0, tiles * SPLIT + CORES - 1), 0, 0], z_send)
        sent(blocks.at[pl.ds(0, nrow - 1), 0], mate_send)

    @pl.when(is_inside)
    def _():
        some_sums(nrow - 1).wait_send()

    @pl.when(is_aide)
    def _():
        some_sums(nrow - 1).wait_send()
        number = len(beside) * topped + 1
        sent(aid.at[pl.ds(0, number), 0, 0, pl.ds(0, kept)], aid_send.at[1])
        if topped:
            sent(blocks.at[pl.ds(0, 3 * len(along_x)), 0], aid_send.at[0])
        else:
            sent(blocks.at[pl.ds(0, len(beside) * CORES), 0], aid_send.at[0])


def on_device(nrow, ncol, flow_tiles, tile_cols, pairs):
    _, tiles, _, width = flow_tiles.shape
    depth = width // SPLIT
    dma = pltpu.SemaphoreType.DMA
    return pl.pallas_call(
        functools.partial(kernel, nrow, ncol),
        out_shape=jax.ShapeDtypeStruct(flow_tiles.shape, jnp.float32),
        in_specs=[pl.BlockSpec(memory_space=pltpu.HBM)] * 2,
        out_specs=pl.BlockSpec(memory_space=pltpu.VMEM),
        scratch_shapes=[
            pltpu.SMEM((1, tiles), jnp.int32),
            pltpu.VMEM((tiles, width, width), jnp.bfloat16),
            pltpu.VMEM((ncol, tiles, SPLIT, depth, width), jnp.bfloat16),
            pltpu.VMEM((nrow, tiles, SPLIT, depth, width), jnp.bfloat16),
            pltpu.VMEM((ncol, tiles, SPLIT, depth, width), jnp.bfloat16),
            pltpu.VMEM((tiles, width, width), jnp.float32),
            pltpu.VMEM((tiles, width, width), jnp.float32),
            pltpu.VMEM((tiles, width), jnp.float32),
            pltpu.VMEM((tiles, width), jnp.float32),
            pltpu.VMEM((nrow, tiles, width), jnp.float32),
            dma,
            dma,
            dma((nrow - CORES, SPLIT)),
            dma((nrow // CORES + (SPLIT - 1) * CORES,)),
            dma,
            dma((2 * SPLIT + 1,)),
            dma((2,)),
            dma((2 * SPLIT,)),
            dma((2,)),
            dma((2,)),
        ],
        compiler_params=pltpu.CompilerParams(
            collective_id=0, has_side_effects=True, vmem_limit_bytes=24 * 1024 * 1024
        ),
        name="cluster_step",
    )(
        pltpu.with_memory_space_constraint(tile_cols, pltpu.HBM),
        pltpu.with_memory_space_constraint(flow_tiles, pltpu.HBM),
    )


def solution(mesh):
    placed = (P("row", "col", None, None), P("row", "col"), P(("row", "col"), None))
    return jax.shard_map(
        functools.partial(on_device, mesh.shape["row"], mesh.shape["col"]),
        mesh=mesh,
        in_specs=placed,
        out_specs=P("row", "col", None, None),
        check_vma=False,
    )
```
